32 devices in a mesh: gx: 4 (over y, core), gy: 2 (over x), gz: 4 (over z).
Axes of the slice: x: 2, y: 2, z: 4, core: 2. Of those that a mesh axis runs over, the one named last changes fastest.
Arguments:
- tokens: bfloat16 [32, 6144], P('gy'), may hold values from -6 to 6
- route: int32 [32, 2], P('gy'), may hold values from 0 to 3, all different within a row; in each aligned block of 16 rows (0 to 15, 16 to 31, ...) at most 12 rows name the same one
- weight_q: int32 [32, 2], P('gy'), may hold values from 1 to 65535
- w_gate: bfloat16 [4, 6144, 16384], P('gx', 'gy', 'gz'), may hold values from -0.078125 to 0.078125
- w_up: bfloat16 [4, 6144, 16384], P('gx', 'gy', 'gz'), may hold values from -0.078125 to 0.078125
- w_down: bfloat16 [4, 16384, 6144], P('gx', 'gz', 'gy'), may hold values from -0.046875 to 0.046875
Outputs:
- mixed: bfloat16 [32, 6144], P('gy', ('gx', 'gz'))
The draws below stay inside these ranges and needn't reach their ends.
Inputs may be any that keep to these rules, and one draw needn't show every extreme that they name: `route`: the 2 entries of a row are different; in each block of 16 rows owned by one index of gy no expert is named by more than 12 rows, a bound that some block reaches.
All inputs are finite; a program needn't handle non-finite values.
Results may differ from the reference program's by a relative error of at most 0.0049.
Values may be sent and summed in bfloat16 or wider, within the bound.
A program may use at most 256 MiB of HBM per device.

```python
import math
import jax
import jax.numpy as jnp
import numpy as np
from jax import lax

D = 6144
FF = 16384
TOK_OWN = 16
TOP = 2
CAP = 12
EXPERTS = 4
TOKENS = 32


def place_ends(drawn, own_key, smallest, largest):
    longest = drawn.shape.index(max(drawn.shape))
    spots = []
    for shift in (0, 1):
        where = [jax.random.randint(jax.random.fold_in(own_key, axis), (), 0, length) for axis, length in enumerate(drawn.shape)]
        where[longest] = (where[longest] + shift) % drawn.shape[longest]
        spots.append(tuple(where))
    return drawn.at[spots[0]].set(smallest).at[spots[1]].set(largest)


def shard_levels(key, shape, cuts, smallest, high):
    gain = 1.0
    for dim, parts in cuts:
        heights = jax.random.uniform(jax.random.fold_in(jax.random.fold_in(key, 6), dim), (parts,), jnp.float32, smallest / len(cuts), high / len(cuts))
        gain = gain * jnp.repeat(jnp.exp(heights), shape[dim] // parts).reshape((-1,) + (1,) * (len(shape) - 1 - dim))
    return gain


def assign_block(key, own, number, rows, count, top, most, slope):
    ranking = jax.random.permutation(key, count)
    heavy_load, usual = load_shares(count, rows * top, most, slope, True), load_shares(count, rows * top, most, slope, False)
    places = jnp.arange(count)

    def named(sizes, offset_by):
        used = int((sizes > 0).sum())
        fixed = max(1, used // 4)
        moved = fixed + (places - fixed + offset_by * (used - fixed)) % max(1, count - fixed)
        return jnp.zeros((count,), jnp.int32).at[ranking[jnp.where(places < fixed, places, moved)]].set(jnp.asarray(sizes, jnp.int32))

    sizes = jnp.where(number % 4 == 0, named(heavy_load, number // 4), named(usual, number - number // 4 - 1))
    mixed = jax.random.permutation(jax.random.fold_in(own, 3), count)
    donor, sink = mixed[0:count // 2 * 2:2], mixed[1:count // 2 * 2:2]
    slack = jnp.minimum(sizes[donor] - 1, most - sizes[sink]) // 2
    slack = jnp.where((donor == ranking[0]) | (sink == ranking[0]) | (sizes[sink] == 0), 0, jnp.maximum(slack, 0))
    moved = jax.random.randint(jax.random.fold_in(own, 4), (count // 2,), 0, 1 << 20) % (slack + 1)
    sizes = sizes.at[donor].add(-moved).at[sink].add(moved)
    labels = jnp.searchsorted(jnp.cumsum(sizes), jnp.arange(rows * top), side="right").astype(jnp.int32)
    table = labels.reshape(top, rows).T
    table = table[jax.random.permutation(jax.random.fold_in(own, 1), rows)]
    offset_by = jax.random.randint(jax.random.fold_in(own, 2), (rows, 1), 0, top)
    return jnp.take_along_axis(table, (jnp.arange(top)[None, :] + offset_by) % top, axis=1)


def load_shares(count, total, bound, lean, full):
    portions = [(1 << 20) // math.isqrt(standing ** lean) + 1 for standing in range(1, count + 1)]
    largest = bound if full else min(bound, max(-(-total // count), total * portions[0] // sum(portions)))
    least = 1 if total - largest >= count - 1 else 0
    given, surplus = [largest] + [least] * (count - 1), total - largest - least * (count - 1)
    while surplus > 0:
        free = [i for i in range(1, count) if given[i] < largest] or [i for i in range(1, count) if given[i] < bound]
        pool, budget = sum([portions[i] for i in free]), surplus
        for i in free:
            extra = min(bound - given[i], max(1, budget * portions[i] // pool), surplus)
            given[i] = given[i] + extra
            surplus = surplus - extra
    return np.array(given)


def scatter_about(key, shape, scale, most, shards=(), kind=jnp.bfloat16):
    array = jax.random.normal(key, shape, jnp.float32) * scale
    if len(shards) > 0:
        array = shard_levels(key, shape, shards, -0.22, 0.18) * array
    return jnp.clip(array, min=-most, max=most).astype(kind)


def setup_inputs(seed: int = 0) -> dict:
    splits = jax.random.split(jax.random.key(seed), 7)
    tokens = scatter_about(splits[0], (TOKENS, D), 1.0, 6.0, ((0, 2),))
    route_keys = jax.random.split(jax.random.fold_in(splits[1], 1), TOKENS // TOK_OWN)
    route_turns = jax.random.permutation(jax.random.fold_in(splits[1], 3), TOKENS // TOK_OWN)
    route = jax.vmap(lambda own, number: assign_block(jax.random.fold_in(splits[1], 2), own, number, TOK_OWN, EXPERTS, TOP, CAP, 2))(route_keys, route_turns).reshape((TOKENS, TOP))
    weight_q = place_ends(jax.random.randint(splits[2], (TOKENS, TOP), 1, 65536), jax.random.fold_in(splits[2], 1), 1, 65535).astype(jnp.int32)
    w_gate = scatter_about(splits[3], (EXPERTS, D, FF), D ** -0.5, 0.078125, ((0, 4), (1, 2), (2, 4)))
    w_up = scatter_about(splits[4], (EXPERTS, D, FF), D ** -0.5, 0.078125, ((0, 4), (1, 2), (2, 4)))
    w_down = scatter_about(splits[5], (EXPERTS, FF, D), FF ** -0.5, 0.046875, ((0, 4), (1, 4), (2, 2)))
    return {"tokens": tokens, "route": route, "weight_q": weight_q, "w_gate": w_gate, "w_up": w_up, "w_down": w_down}


def slot_table(owner_ids, expert):
    hits = (owner_ids == expert).astype(jnp.int32)
    routed = jnp.sum(hits, axis=-1)
    slot_index = jnp.cumsum(routed, axis=1) - 1
    columns = jnp.arange(CAP, dtype=jnp.int32)
    placing = (slot_index[:, None, :] == columns[None, :, None]) & (routed[:, None, :] > 0)
    return hits, placing


def reference(tokens, route, weight_q, w_gate, w_up, w_down):
    groups = TOKENS // TOK_OWN
    owner_ids = route.reshape(groups, TOK_OWN, TOP)
    owned = tokens.reshape(groups, TOK_OWN, D)
    weights_f = weight_q.astype(jnp.float32).reshape(groups, TOK_OWN, TOP)
    shares = weights_f / jnp.sum(weights_f, axis=-1, keepdims=True)
    positions = jnp.arange(TOK_OWN, dtype=jnp.int32)

    def one_expert(total, expert):
        hits, placing = slot_table(owner_ids, expert)
        place_full = placing.astype(jnp.float32)
        picked = jnp.sum(placing.astype(jnp.int32) * positions[None, None, :], axis=-1).astype(jnp.int32)
        filled = jnp.any(placing, axis=-1)
        rows = jnp.take_along_axis(owned, picked[:, :, None], axis=1)
        rows = rows * filled[:, :, None].astype(jnp.bfloat16)
        flat = rows.reshape(groups * CAP, D)
        gate = jnp.dot(flat, w_gate[expert], preferred_element_type=jnp.float32)
        upper = jnp.dot(flat, w_up[expert], preferred_element_type=jnp.float32)
        hidden = (jax.nn.silu(gate) * upper).astype(jnp.bfloat16)
        result = jnp.dot(hidden, w_down[expert], preferred_element_type=jnp.float32)
        token_gate = jnp.sum(hits.astype(jnp.float32) * shares, axis=-1)
        slot_gate = jnp.einsum("gct,gt->gc", place_full, token_gate, precision=lax.Precision.HIGHEST)
        weighted = slot_gate[:, :, None] * result.reshape(groups, CAP, D)
        back = jnp.einsum("gct,gcd->gtd", place_full, weighted, precision=lax.Precision.HIGHEST)
        return total + back, None

    start = jnp.zeros((groups, TOK_OWN, D), jnp.float32)
    total, _ = lax.scan(one_expert, start, jnp.arange(EXPERTS, dtype=jnp.int32))
    return total.reshape(TOKENS, D).astype(jnp.bfloat16)
```

```python
import functools

import jax
import jax.numpy as jnp
from jax import lax
from jax.experimental import pallas as pl
from jax.experimental.pallas import tpu as pltpu
from jax.sharding import PartitionSpec as P

CAP = 12
SLOTS = 16
STEPS = 8
RING = 5
AHEAD = 4
MESH = pl.DeviceIdType.MESH
F32, BF16 = jnp.float32, jnp.bfloat16


def plain(tokens, route, weight_q, w_gate, w_up, w_down):
    expert = lax.axis_index("gx")
    width_z = lax.axis_size("gz")
    owners = lax.axis_size("gy")
    hits = (route == expert).astype(jnp.int32)
    routed = jnp.sum(hits, axis=1)
    slot_index = jnp.cumsum(routed) - 1
    columns = jnp.arange(CAP, dtype=jnp.int32)
    placing = (slot_index[None, :] == columns[:, None]) & (routed[None, :] > 0)
    place_half = placing.astype(jnp.bfloat16)
    place_full = placing.astype(jnp.float32)
    outgoing = jnp.dot(place_half, tokens, preferred_element_type=jnp.float32).astype(jnp.bfloat16)
    weights_f = weight_q.astype(jnp.float32)
    shares = weights_f / jnp.sum(weights_f, axis=1, keepdims=True)
    token_gate = jnp.sum(hits.astype(jnp.float32) * shares, axis=1)
    slot_gate = jnp.dot(place_full, token_gate, precision=lax.Precision.HIGHEST)
    depth = w_gate.shape[1]
    half = outgoing.reshape(CAP, owners, depth).transpose(1, 0, 2)
    piece = lax.all_to_all(half, "gy", split_axis=0, concat_axis=0, tiled=True)
    piece = piece.reshape(owners * CAP, depth)
    gate = jnp.dot(piece, w_gate[0], preferred_element_type=jnp.float32)
    upper = jnp.dot(piece, w_up[0], preferred_element_type=jnp.float32)
    both = lax.psum_scatter(jnp.stack([gate, upper]), "gy", scatter_dimension=2, tiled=True)
    hidden = (jax.nn.silu(both[0]) * both[1]).astype(jnp.bfloat16)
    down_local = w_down[0]
    partial_value = jnp.dot(
        lax.all_gather(hidden, "gy", axis=1, tiled=True),
        down_local,
        preferred_element_type=jnp.float32,
    )
    portion = CAP // width_z
    column_width = partial_value.shape[1]
    blocks = partial_value.reshape(owners, width_z, portion, column_width)
    narrowed = lax.psum_scatter(blocks, "gz", scatter_dimension=1, tiled=True)
    arrived = lax.all_to_all(narrowed, "gy", split_axis=0, concat_axis=1, tiled=True)
    full = jnp.transpose(arrived[0], (1, 0, 2)).reshape(portion, owners * column_width)
    first = lax.axis_index("gz") * portion
    gate_part = lax.dynamic_slice_in_dim(slot_gate, first, portion, 0)
    place_part = lax.dynamic_slice_in_dim(place_full, first, portion, 0)
    weighted = gate_part[:, None] * full
    contribution = jnp.dot(place_part.T, weighted, precision=lax.Precision.HIGHEST)
    result = lax.psum_scatter(contribution, ("gx", "gz"), scatter_dimension=1, tiled=True)
    return result.astype(jnp.bfloat16)


def kernel(sizes, tok_hbm, route_hbm, wq_hbm, wg_hbm, wu_hbm, wd_hbm, out_ref,
           tok, route, wq, gbuf, ubuf, dbuf_a, dbuf_b, xs, xsend, own, psend, precv,
           hid, acc, sbuf, rbuf, sem_in, sem_g, sem_u, sem_a, sem_b,
           tok_ss, tok_rs, ex_ss, ex_rs, out_ss, out_rs):
    nx, ny, nz = sizes
    gx, gy, gz = lax.axis_index("gx"), lax.axis_index("gy"), lax.axis_index("gz")
    other = 1 - gy
    depth, ffl = wg_hbm.shape[1], wg_hbm.shape[2]
    cn = ffl // STEPS
    half_steps = STEPS // 2
    width = wd_hbm.shape[2]
    nb = nx * nz // ny
    bw = width // nb
    token_rows = tok.shape[0]
    kb = ffl // 2

    def pair(j):
        slot = lax.rem(j, RING)
        cols = pl.ds(pl.multiple_of(j * cn, cn), cn)
        return (pltpu.make_async_copy(wg_hbm.at[0, :, cols], gbuf.at[slot], sem_g.at[slot]),
                pltpu.make_async_copy(wu_hbm.at[0, :, cols], ubuf.at[slot], sem_u.at[slot]))

    def down_a(j):
        rows = pl.ds(pl.multiple_of(j * cn, cn), cn)
        return pltpu.make_async_copy(wd_hbm.at[0, rows, :], dbuf_a.at[j], sem_a.at[j])

    low = gz < nz // 2

    def block_of(i):
        per = nb // nz
        k = i // per
        z = jnp.where(low, nz - 1 - k, k)
        return lax.rem(i, per) * nz + z, lax.rem(i, per), z

    def down_b(i):
        b, _, _ = block_of(i)
        cols = pl.ds(pl.multiple_of(b * bw, 128), bw)
        return pltpu.make_async_copy(wd_hbm.at[0, kb:, cols], dbuf_b.at[i], sem_b.at[i])

    ins = [pltpu.make_async_copy(tok_hbm, tok, sem_in.at[0]),
           pltpu.make_async_copy(route_hbm, route, sem_in.at[1]),
           pltpu.make_async_copy(wq_hbm, wq, sem_in.at[2])]
    for c in ins:
        c.start()
    for j in range(AHEAD):
        for c in pair(j):
            c.start()

    mine = gx * nz + gz
    src_y = mine // nb
    gx_first = gy * (nb // nz)
    barrier = pltpu.get_barrier_semaphore()
    pl.semaphore_signal(barrier, inc=1, device_id=(gx, other, gz), device_id_type=MESH)
    for e in range(nx):
        for z in range(nz):
            @pl.when(jnp.logical_not((e == gx) & (src_y == gy) & (z == gz)))
            def _():
                pl.semaphore_signal(barrier, inc=1, device_id=(e, src_y, z), device_id_type=MESH)

    for c in ins:
        c.wait()

    lane_t = lax.broadcasted_iota(jnp.int32, (token_rows, token_rows), 1)
    sub_t = lax.broadcasted_iota(jnp.int32, (token_rows, token_rows), 0)
    eye = (lane_t == sub_t).astype(F32)
    upto = (lane_t <= sub_t).astype(F32)
    r0, r1 = route[0:1, :], route[1:2, :]
    w0, w1 = wq[0:1, :].astype(F32), wq[1:2, :].astype(F32)
    total = w0 + w1
    s0, s1 = w0 / total, w1 / total

    def hit_row(e):
        return ((r0 == e) | (r1 == e)).astype(F32)

    hr = hit_row(gx)
    hc = jnp.sum(eye * hr, axis=1, keepdims=True)
    upper_tri = (sub_t <= lane_t).astype(F32)
    slot_row = jnp.sum(upper_tri * hc, axis=0, keepdims=True) - 1.0
    slots_sub = lax.broadcasted_iota(jnp.int32, (SLOTS, token_rows), 0).astype(F32)
    place = ((slot_row == slots_sub) & (hr > 0.0)).astype(F32).astype(BF16)

    spreads = []
    slots_lane = lax.broadcasted_iota(jnp.int32, (token_rows, SLOTS), 1).astype(F32)
    for e in range(nx):
        h = hit_row(e)
        g = jnp.where(r0 == e, s0, 0.0) + jnp.where(r1 == e, s1, 0.0)
        slot_col = jnp.sum(upto * h, axis=1, keepdims=True) - 1.0
        gate_col = jnp.sum(eye * g, axis=1, keepdims=True)
        hit_col = jnp.sum(eye * h, axis=1, keepdims=True)
        spreads.append(jnp.where((slot_col == slots_lane) & (hit_col > 0.0), gate_col, 0.0))

    my_rows = pl.ds(pl.multiple_of(gy * SLOTS, SLOTS), SLOTS)
    piece = depth // 3
    for q in range(3):
        theirs = pl.ds(pl.multiple_of(other * depth + q * piece, 128), piece)
        xsend[:, q * piece:(q + 1) * piece] = jnp.dot(
            place, tok[:, theirs], preferred_element_type=F32).astype(BF16)
    for q in range(3):
        ours = pl.ds(pl.multiple_of(gy * depth + q * piece, 128), piece)
        xs[my_rows, q * piece:(q + 1) * piece] = jnp.dot(
            place, tok[:, ours], preferred_element_type=F32).astype(BF16)

    self_dest = src_y == gy
    pl.semaphore_wait(barrier, ny * nb + 1 - self_dest.astype(jnp.int32))

    partner = (gx, other, gz)
    tok_copy = pltpu.make_async_remote_copy(
        src_ref=xsend, dst_ref=xs.at[my_rows, :], send_sem=tok_ss, recv_sem=tok_rs,
        device_id=partner, device_id_type=MESH)
    tok_copy.start()
    acc[...] = jnp.zeros_like(acc)
    tok_copy.wait()

    def exchange(j):
        return pltpu.make_async_remote_copy(
            src_ref=psend.at[j], dst_ref=precv.at[j], send_sem=ex_ss.at[j], recv_sem=ex_rs.at[j],
            device_id=partner, device_id_type=MESH)

    def project(j, carry):
        slot = lax.rem(j, RING)
        cg, cu = pair(j)

        @pl.when(j + AHEAD < STEPS)
        def _():
            for c in pair(j + AHEAD):
                c.start()

        @pl.when((j + AHEAD >= STEPS) & (j + AHEAD < STEPS + half_steps // 2))
        def _():
            first = (j + AHEAD - STEPS) * 2
            down_a(first).start()
            down_a(first + 1).start()

        @pl.when(j + AHEAD >= STEPS + half_steps // 2)
        def _():
            per = nb // (half_steps - half_steps // 2)
            first = (j + AHEAD - STEPS - half_steps // 2) * per
            for t in range(per):
                down_b(first + t).start()

        cg.wait()
        g = jnp.dot(xs[...], gbuf[slot], preferred_element_type=F32)
        own[j, 0] = g
        psend[j, 0] = g.astype(BF16)
        cu.wait()
        u = jnp.dot(xs[...], ubuf[slot], preferred_element_type=F32)
        own[j, 1] = u
        psend[j, 1] = u.astype(BF16)
        exchange(j).start()
        return carry

    lax.fori_loop(0, STEPS, project, 0)

    def hidden(j):
        exchange(j).wait_recv()
        g = own[j, 0] + precv[j, 0].astype(F32)
        u = own[j, 1] + precv[j, 1].astype(F32)
        return (g * jax.nn.sigmoid(g) * u).astype(BF16)

    nsub = 4
    sw = width // nsub

    def first_half(j, carry):
        h = hidden(j)
        down_a(j).wait()
        for q in range(nsub):
            cols = slice(q * sw, (q + 1) * sw)
            acc[:, cols] += jnp.dot(h, dbuf_a[j, :, cols], preferred_element_type=F32)
        return carry

    lax.fori_loop(0, half_steps, first_half, 0)
    for j in range(half_steps, STEPS):
        hid[:, (j - half_steps) * cn:(j - half_steps + 1) * cn] = hidden(j)

    def out_copy(i, o):
        _, c, z = block_of(i)
        here = gx * nz + gz
        return pltpu.make_async_remote_copy(
            src_ref=sbuf.at[i, o], dst_ref=rbuf.at[here], send_sem=out_ss.at[i, o],
            recv_sem=out_rs.at[here], device_id=(gx_first + c, o, z), device_id_type=MESH)

    def to_self(i, o):
        _, c, z = block_of(i)
        return (gx_first + c == gx) & (o == gy) & (z == gz)

    def second_half(i, carry):
        b, c, z = block_of(i)
        cols = pl.ds(pl.multiple_of(b * bw, 128), bw)
        down_b(i).wait()
        y = acc[:, cols] + jnp.dot(hid[...], dbuf_b[i], preferred_element_type=F32)
        yb = y.astype(BF16)
        for o in range(ny):
            part = yb[o * SLOTS:(o + 1) * SLOTS]
            sbuf[i, o] = part

            @pl.when(to_self(i, o))
            def _():
                rbuf[gx * nz + gz] = part

            @pl.when(jnp.logical_not(to_self(i, o)))
            def _():
                out_copy(i, o).start()
        return carry

    lax.fori_loop(0, nb, second_half, 0)

    sums = []
    for e in range(nx):
        s = None
        for z in range(nz):
            @pl.when(jnp.logical_not((e == gx) & (src_y == gy) & (z == gz)))
            def _():
                pltpu.make_async_remote_copy(
                    src_ref=sbuf.at[0, 0], dst_ref=rbuf.at[e * nz + z], send_sem=out_ss.at[0, 0],
                    recv_sem=out_rs.at[e * nz + z], device_id=(e, src_y, z),
                    device_id_type=MESH).wait_recv()
    for e in range(nx):
        s = rbuf[e * nz].astype(F32)
        for z in range(1, nz):
            s = s + rbuf[e * nz + z].astype(F32)
        sums.append(jnp.dot(spreads[e], s, precision=lax.Precision.HIGHEST,
                            preferred_element_type=F32))
    out_ref[...] = functools.reduce(lambda a, b: a + b, sums).astype(out_ref.dtype)

    def drain(j, carry):
        exchange(j).wait_send()
        return carry

    lax.fori_loop(0, STEPS, drain, 0)

    def drain_out(i, carry):
        for o in range(ny):
            @pl.when(jnp.logical_not(to_self(i, o)))
            def _():
                out_copy(i, o).wait_send()
        return carry

    lax.fori_loop(0, nb, drain_out, 0)


def fused(sizes, tokens, route, weight_q, w_gate, w_up, w_down):
    nx, ny, nz = sizes
    depth, ffl = w_gate.shape[1], w_gate.shape[2]
    width = w_down.shape[2]
    cn = ffl // STEPS
    nb = nx * nz // ny
    bw = width // nb
    rows = ny * SLOTS
    dma = pltpu.SemaphoreType.DMA
    hbm = pl.BlockSpec(memory_space=pl.ANY)
    return pl.pallas_call(
        functools.partial(kernel, sizes),
        out_shape=jax.ShapeDtypeStruct((tokens.shape[0], bw), BF16),
        in_specs=[hbm] * 6,
        out_specs=pl.BlockSpec(memory_space=pltpu.VMEM),
        scratch_shapes=[
            pltpu.VMEM(tokens.shape, BF16),
            pltpu.VMEM(route.shape[::-1], jnp.int32),
            pltpu.VMEM(route.shape[::-1], jnp.int32),
            pltpu.VMEM((RING, depth, cn), BF16),
            pltpu.VMEM((RING, depth, cn), BF16),
            pltpu.VMEM((STEPS // 2, cn, width), BF16),
            pltpu.VMEM((nb, ffl // 2, bw), BF16),
            pltpu.VMEM((rows, depth), BF16),
            pltpu.VMEM((SLOTS, depth), BF16),
            pltpu.VMEM((STEPS, 2, rows, cn), F32),
            pltpu.VMEM((STEPS, 2, rows, cn), BF16),
            pltpu.VMEM((STEPS, 2, rows, cn), BF16),
            pltpu.VMEM((rows, ffl // 2), BF16),
            pltpu.VMEM((rows, width), F32),
            pltpu.VMEM((nb, ny, SLOTS, bw), BF16),
            pltpu.VMEM((nx * nz, SLOTS, bw), BF16),
            dma((3,)), dma((RING,)), dma((RING,)), dma((STEPS // 2,)), dma((nb,)),
            dma, dma, dma((STEPS,)), dma((STEPS,)), dma((nb, ny)), dma((nx * nz,)),
        ],
        compiler_params=pltpu.CompilerParams(
            collective_id=0, has_side_effects=True, vmem_limit_bytes=67043328),
        name="routed_ffn",
    )(tokens, route.T, weight_q.T, w_gate, w_up, w_down)


def solution(mesh):
    in_specs = (
        P("gy", None),
        P("gy", None),
        P("gy", None),
        P("gx", "gy", "gz"),
        P("gx", "gy", "gz"),
        P("gx", "gz", "gy"),
    )
    out_specs = P("gy", ("gx", "gz"))
    sizes = tuple(mesh.shape[name] for name in ("gx", "gy", "gz"))
    body = functools.partial(fused, sizes) if sizes[1] == 2 else plain
    return jax.shard_map(
        body, mesh=mesh, in_specs=in_specs, out_specs=out_specs, check_vma=False
    )
```

```python
import functools

import jax
import jax.numpy as jnp
from jax import lax
from jax.experimental import pallas as pl
from jax.experimental.pallas import tpu as pltpu
from jax.sharding import PartitionSpec as P

CAP = 12
LOW = 8
PIECE = 16
ROWS = 24
STEPS = 8
EARLY = 4
RING = 5
LAG = 3
FIRST = 2
MESH = pl.DeviceIdType.MESH
F32, BF16 = jnp.float32, jnp.bfloat16


def plain(tokens, route, weight_q, w_gate, w_up, w_down):
    expert = lax.axis_index("gx")
    width_z = lax.axis_size("gz")
    owners = lax.axis_size("gy")
    hits = (route == expert).astype(jnp.int32)
    routed = jnp.sum(hits, axis=1)
    slot_index = jnp.cumsum(routed) - 1
    columns = jnp.arange(CAP, dtype=jnp.int32)
    placing = (slot_index[None, :] == columns[:, None]) & (routed[None, :] > 0)
    place_half = placing.astype(jnp.bfloat16)
    place_full = placing.astype(jnp.float32)
    outgoing = jnp.dot(place_half, tokens, preferred_element_type=jnp.float32).astype(jnp.bfloat16)
    weights_f = weight_q.astype(jnp.float32)
    shares = weights_f / jnp.sum(weights_f, axis=1, keepdims=True)
    token_gate = jnp.sum(hits.astype(jnp.float32) * shares, axis=1)
    slot_gate = jnp.dot(place_full, token_gate, precision=lax.Precision.HIGHEST)
    depth = w_gate.shape[1]
    half = outgoing.reshape(CAP, owners, depth).transpose(1, 0, 2)
    piece = lax.all_to_all(half, "gy", split_axis=0, concat_axis=0, tiled=True)
    piece = piece.reshape(owners * CAP, depth)
    gate = jnp.dot(piece, w_gate[0], preferred_element_type=jnp.float32)
    upper = jnp.dot(piece, w_up[0], preferred_element_type=jnp.float32)
    both = lax.psum_scatter(jnp.stack([gate, upper]), "gy", scatter_dimension=2, tiled=True)
    hidden = (jax.nn.silu(both[0]) * both[1]).astype(jnp.bfloat16)
    down_local = w_down[0]
    partial_value = jnp.dot(
        lax.all_gather(hidden, "gy", axis=1, tiled=True),
        down_local,
        preferred_element_type=jnp.float32,
    )
    portion = CAP // width_z
    column_width = partial_value.shape[1]
    blocks = partial_value.reshape(owners, width_z, portion, column_width)
    narrowed = lax.psum_scatter(blocks, "gz", scatter_dimension=1, tiled=True)
    arrived = lax.all_to_all(narrowed, "gy", split_axis=0, concat_axis=1, tiled=True)
    full = jnp.transpose(arrived[0], (1, 0, 2)).reshape(portion, owners * column_width)
    first = lax.axis_index("gz") * portion
    gate_part = lax.dynamic_slice_in_dim(slot_gate, first, portion, 0)
    place_part = lax.dynamic_slice_in_dim(place_full, first, portion, 0)
    weighted = gate_part[:, None] * full
    contribution = jnp.dot(place_part.T, weighted, precision=lax.Precision.HIGHEST)
    result = lax.psum_scatter(contribution, ("gx", "gz"), scatter_dimension=1, tiled=True)
    return result.astype(jnp.bfloat16)


def kernel(sizes, tok_hbm, route_hbm, wq_hbm, wg_hbm, wu_hbm, wd_hbm, out_ref,
           tok, route, wq, gbuf, ubuf, dbuf_a, dbuf_b, xb, xsend, xs, part, precv,
           hid, late, acc, sbuf, rbuf, sem_in, sem_g, sem_u, sem_a, sem_b, stage,
           tok_ss, tok_rs, ex_ss, ex_rs, hid_ss, hid_rs, out_ss, out_rs):
    nx, ny, nz = sizes
    gx, gy, gz = lax.axis_index("gx"), lax.axis_index("gy"), lax.axis_index("gz")
    other = 1 - gy
    depth, ffl = wg_hbm.shape[1], wg_hbm.shape[2]
    cn = ffl // STEPS
    hw = cn // ny
    width = wd_hbm.shape[2]
    nb = nx * nz // ny
    bw = width // nb
    token_rows = tok.shape[0]
    kb = EARLY * cn
    partner = (gx, other, gz)

    def pair(j):
        slot = lax.rem(j, RING)
        cols = pl.ds(pl.multiple_of(j * cn, cn), cn)
        return (pltpu.make_async_copy(wg_hbm.at[0, :, cols], gbuf.at[slot], sem_g.at[slot]),
                pltpu.make_async_copy(wu_hbm.at[0, :, cols], ubuf.at[slot], sem_u.at[slot]))

    def down_a(j):
        rows = pl.ds(pl.multiple_of(j * cn, cn), cn)
        return pltpu.make_async_copy(wd_hbm.at[0, rows, :], dbuf_a.at[j], sem_a.at[j])

    per = nb // nz

    def block_of(i):
        z = jnp.where(gz < nz // 2, nz - 1 - i // per, i // per)
        return lax.rem(i, per) * nz + z, lax.rem(i, per), z

    def down_b(i):
        b, _, _ = block_of(i)
        cols = pl.ds(pl.multiple_of(b * bw, 128), bw)
        return pltpu.make_async_copy(wd_hbm.at[0, kb:, cols], dbuf_b.at[i], sem_b.at[i])

    ins = [pltpu.make_async_copy(tok_hbm, tok, sem_in.at[0]),
           pltpu.make_async_copy(route_hbm, route, sem_in.at[1]),
           pltpu.make_async_copy(wq_hbm, wq, sem_in.at[2])]
    for c in ins:
        c.start()
    for j in range(RING):
        for c in pair(j):
            c.start()
    for j in range(FIRST):
        down_a(j).start()

    near_count = (nx - 1) + (ny - 1) + (gz > 0).astype(jnp.int32) + (gz < nz - 1).astype(jnp.int32)

    def signal_near(sem):
        pl.semaphore_signal(sem, inc=1, device_id=partner, device_id_type=MESH)
        for d in range(1, nx):
            pl.semaphore_signal(sem, inc=1, device_id=(lax.rem(gx + d, nx), gy, gz), device_id_type=MESH)

        @pl.when(gz > 0)
        def _():
            pl.semaphore_signal(sem, inc=1, device_id=(gx, gy, gz - 1), device_id_type=MESH)

        @pl.when(gz < nz - 1)
        def _():
            pl.semaphore_signal(sem, inc=1, device_id=(gx, gy, gz + 1), device_id_type=MESH)

    barrier = pltpu.get_barrier_semaphore()
    signal_near(barrier)

    for c in ins:
        c.wait()

    lane_t = lax.broadcasted_iota(jnp.int32, (token_rows, token_rows), 1)
    sub_t = lax.broadcasted_iota(jnp.int32, (token_rows, token_rows), 0)
    eye = (lane_t == sub_t).astype(F32)
    upto = (lane_t <= sub_t).astype(F32)
    since = (sub_t <= lane_t).astype(F32)
    r0, r1 = route[0:1, :], route[1:2, :]
    shift = gy.astype(F32) * (PIECE - CAP)

    def hit_row(e):
        return ((r0 == e) | (r1 == e)).astype(F32)

    def row_of(slot):
        return jnp.where(slot < LOW, slot, slot + shift)

    hr = hit_row(gx)
    hc = jnp.sum(eye * hr, axis=1, keepdims=True)
    slot_row = row_of(jnp.sum(since * hc, axis=0, keepdims=True) - 1.0)
    rows_sub = lax.broadcasted_iota(jnp.int32, (PIECE, token_rows), 0).astype(F32)
    place = ((slot_row == rows_sub) & (hr > 0.0)).astype(F32).astype(BF16)

    thirds = 3
    span = depth // thirds
    for q in range(thirds):
        theirs = pl.ds(pl.multiple_of(other * depth + q * span, 128), span)
        xsend[:, q * span:(q + 1) * span] = jnp.dot(
            place, tok[:, theirs], preferred_element_type=F32).astype(BF16)

    pl.semaphore_wait(barrier, near_count)
    tok_copy = pltpu.make_async_remote_copy(
        src_ref=xsend, dst_ref=xb.at[gy], send_sem=tok_ss, recv_sem=tok_rs,
        device_id=partner, device_id_type=MESH)
    tok_copy.start()
    signal_near(stage.at[0])

    for q in range(thirds):
        ours = pl.ds(pl.multiple_of(gy * depth + q * span, 128), span)
        xb[gy, :, q * span:(q + 1) * span] = jnp.dot(
            place, tok[:, ours], preferred_element_type=F32).astype(BF16)
    acc[...] = jnp.zeros_like(acc)

    w0, w1 = wq[0:1, :].astype(F32), wq[1:2, :].astype(F32)
    total = w0 + w1
    s0, s1 = w0 / total, w1 / total
    spreads = []
    rows_lane = lax.broadcasted_iota(jnp.int32, (token_rows, PIECE), 1).astype(F32)
    for e in range(nx):
        h = hit_row(e)
        g = jnp.where(r0 == e, s0, 0.0) + jnp.where(r1 == e, s1, 0.0)
        slot_col = row_of(jnp.sum(upto * h, axis=1, keepdims=True) - 1.0)
        gate_col = jnp.sum(eye * g, axis=1, keepdims=True)
        hit_col = jnp.sum(eye * h, axis=1, keepdims=True)
        spreads.append(jnp.where((slot_col == rows_lane) & (hit_col > 0.0), gate_col, 0.0))

    tok_copy.wait()
    for q in range(thirds):
        cols = slice(q * span, (q + 1) * span)
        x0, x1 = xb[0, :, cols].astype(F32), xb[1, :, cols].astype(F32)
        xs[:, cols] = jnp.concatenate(
            [x0[:LOW], x1[:LOW], x0[LOW:] + x1[LOW:]], axis=0).astype(BF16)

    def exchange(j):
        return pltpu.make_async_remote_copy(
            src_ref=part.at[j, other], dst_ref=precv.at[j], send_sem=ex_ss.at[j],
            recv_sem=ex_rs.at[j], device_id=partner, device_id_type=MESH)

    def share(j):
        return pltpu.make_async_remote_copy(
            src_ref=hid.at[j, gy], dst_ref=hid.at[j, gy], send_sem=hid_ss.at[j],
            recv_sem=hid_rs.at[j], device_id=partner, device_id_type=MESH)

    def finish(j):
        exchange(j).wait_recv()
        g = part[j, gy, 0] + precv[j, 0]
        u = part[j, gy, 1] + precv[j, 1]
        hid[j, gy] = (g * jax.nn.sigmoid(g) * u).astype(BF16)
        share(j).start()

    def project(j, carry):
        @pl.when(j < nz)
        def _():
            pl.semaphore_wait(stage.at[j], near_count)

        @pl.when(j < nz - 1)
        def _():
            signal_near(stage.at[j + 1])

        slot = lax.rem(j, RING)
        cg, cu = pair(j)
        cg.wait()
        g = jnp.dot(xs[...], gbuf[slot], preferred_element_type=F32)
        for h in range(ny):
            part[j, h, 0] = g[:, h * hw:(h + 1) * hw]
        cu.wait()
        u = jnp.dot(xs[...], ubuf[slot], preferred_element_type=F32)
        for h in range(ny):
            part[j, h, 1] = u[:, h * hw:(h + 1) * hw]
        exchange(j).start()

        @pl.when(j + RING < STEPS)
        def _():
            for c in pair(j + RING):
                c.start()

        @pl.when(j + RING == STEPS - 1)
        def _():
            for t in range(FIRST, EARLY):
                down_a(t).start()
            for t in range(nb):
                down_b(t).start()

        @pl.when(j >= LAG)
        def _():
            finish(j - LAG)
        return carry

    lax.fori_loop(0, STEPS, project, 0)

    nsub = 4
    sw = width // nsub

    def first_part(j, carry):
        @pl.when(j < LAG)
        def _():
            finish(STEPS - LAG + j)

        share(j).wait_recv()
        down_a(j).wait()
        for q in range(nsub):
            cols = slice(q * sw, (q + 1) * sw)
            y = acc[:, cols]
            for h in range(ny):
                y = y + jnp.dot(hid[j, h], dbuf_a[j, h * hw:(h + 1) * hw, cols],
                                preferred_element_type=F32)
            acc[:, cols] = y
        return carry

    lax.fori_loop(0, EARLY, first_part, 0)
    for j in range(EARLY, STEPS):
        share(j).wait_recv()
        for h in range(ny):
            start = (j - EARLY) * cn + h * hw
            late[:, start:start + hw] = hid[j, h]

    def out_copy(i, o):
        _, c, z = block_of(i)
        here = gx * nz + gz
        return pltpu.make_async_remote_copy(
            src_ref=sbuf.at[i, o], dst_ref=rbuf.at[here], send_sem=out_ss.at[i, o],
            recv_sem=out_rs.at[here], device_id=(gy * per + c, o, z), device_id_type=MESH)

    def to_self(i, o):
        _, c, z = block_of(i)
        return (gy * per + c == gx) & (o == gy) & (z == gz)

    def second_part(i, carry):
        b, c, z = block_of(i)
        cols = pl.ds(pl.multiple_of(b * bw, 128), bw)
        down_b(i).wait()
        y = acc[:, cols] + jnp.dot(late[...], dbuf_b[i], preferred_element_type=F32)
        for o in range(ny):
            sent = jnp.concatenate([y[o * LOW:(o + 1) * LOW], y[ny * LOW:]], axis=0).astype(BF16)
            sbuf[i, o] = sent

            @pl.when(to_self(i, o))
            def _():
                rbuf[gx * nz + gz] = sent

            @pl.when(jnp.logical_not(to_self(i, o)))
            def _():
                out_copy(i, o).start()
        return carry

    lax.fori_loop(0, nb, second_part, 0)

    src_y = (gx * nz + gz) // nb
    for e in range(nx):
        for z in range(nz):
            @pl.when(jnp.logical_not((e == gx) & (src_y == gy) & (z == gz)))
            def _():
                pltpu.make_async_remote_copy(
                    src_ref=sbuf.at[0, 0], dst_ref=rbuf.at[e * nz + z], send_sem=out_ss.at[0, 0],
                    recv_sem=out_rs.at[e * nz + z], device_id=(e, src_y, z),
                    device_id_type=MESH).wait_recv()
    sums = []
    for e in range(nx):
        s = rbuf[e * nz].astype(F32)
        for z in range(1, nz):
            s = s + rbuf[e * nz + z].astype(F32)
        sums.append(jnp.dot(spreads[e], s, precision=lax.Precision.HIGHEST,
                            preferred_element_type=F32))
    out_ref[...] = functools.reduce(lambda a, b: a + b, sums).astype(out_ref.dtype)

    def drain(j, carry):
        exchange(j).wait_send()
        share(j).wait_send()
        return carry

    lax.fori_loop(0, STEPS, drain, 0)

    def drain_out(i, carry):
        for o in range(ny):
            @pl.when(jnp.logical_not(to_self(i, o)))
            def _():
                out_copy(i, o).wait_send()
        return carry

    lax.fori_loop(0, nb, drain_out, 0)


def fused(sizes, tokens, route, weight_q, w_gate, w_up, w_down):
    nx, ny, nz = sizes
    depth, ffl = w_gate.shape[1], w_gate.shape[2]
    width = w_down.shape[2]
    cn = ffl // STEPS
    hw = cn // ny
    nb = nx * nz // ny
    bw = width // nb
    rest = ffl - EARLY * cn
    dma = pltpu.SemaphoreType.DMA
    hbm = pl.BlockSpec(memory_space=pl.ANY)
    return pl.pallas_call(
        functools.partial(kernel, sizes),
        out_shape=jax.ShapeDtypeStruct((tokens.shape[0], bw), BF16),
        in_specs=[hbm] * 6,
        out_specs=pl.BlockSpec(memory_space=pltpu.VMEM),
        scratch_shapes=[
            pltpu.VMEM(tokens.shape, BF16),
            pltpu.VMEM(route.shape[::-1], jnp.int32),
            pltpu.VMEM(route.shape[::-1], jnp.int32),
            pltpu.VMEM((RING, depth, cn), BF16),
            pltpu.VMEM((RING, depth, cn), BF16),
            pltpu.VMEM((EARLY, cn, width), BF16),
            pltpu.VMEM((nb, rest, bw), BF16),
            pltpu.VMEM((ny, PIECE, depth), BF16),
            pltpu.VMEM((PIECE, depth), BF16),
            pltpu.VMEM((ROWS, depth), BF16),
            pltpu.VMEM((STEPS, ny, 2, ROWS, hw), F32),
            pltpu.VMEM((STEPS, 2, ROWS, hw), F32),
            pltpu.VMEM((STEPS, ny, ROWS, hw), BF16),
            pltpu.VMEM((ROWS, rest), BF16),
            pltpu.VMEM((ROWS, width), F32),
            pltpu.VMEM((nb, ny, PIECE, bw), BF16),
            pltpu.VMEM((nx * nz, PIECE, bw), BF16),
            dma((3,)), dma((RING,)), dma((RING,)), dma((EARLY,)), dma((nb,)),
            pltpu.SemaphoreType.REGULAR((nz,)),
            dma, dma, dma((STEPS,)), dma((STEPS,)), dma((STEPS,)), dma((STEPS,)),
            dma((nb, ny)), dma((nx * nz,)),
        ],
        compiler_params=pltpu.CompilerParams(
            collective_id=0, has_side_effects=True, vmem_limit_bytes=67043328),
        name="routed_ffn",
    )(tokens, route.T, weight_q.T, w_gate, w_up, w_down)


def solution(mesh):
    in_specs = (
        P("gy", None),
        P("gy", None),
        P("gy", None),
        P("gx", "gy", "gz"),
        P("gx", "gy", "gz"),
        P("gx", "gz", "gy"),
    )
    out_specs = P("gy", ("gx", "gz"))
    sizes = tuple(mesh.shape[name] for name in ("gx", "gy", "gz"))
    body = functools.partial(fused, sizes) if sizes[1] == 2 else plain
    return jax.shard_map(
        body, mesh=mesh, in_specs=in_specs, out_specs=out_specs, check_vma=False
    )
```

```python
import functools

import jax
import jax.numpy as jnp
from jax import lax
from jax.experimental import pallas as pl
from jax.experimental.pallas import tpu as pltpu
from jax.sharding import PartitionSpec as P

CAP = 12
LOW = 8
PIECE = 16
ROWS = 24
STEPS = 8
EARLY = 6
RING = 5
LAG = 3
MESH = pl.DeviceIdType.MESH
F32, BF16 = jnp.float32, jnp.bfloat16


def plain(tokens, route, weight_q, w_gate, w_up, w_down):
    expert = lax.axis_index("gx")
    width_z = lax.axis_size("gz")
    owners = lax.axis_size("gy")
    hits = (route == expert).astype(jnp.int32)
    routed = jnp.sum(hits, axis=1)
    slot_index = jnp.cumsum(routed) - 1
    columns = jnp.arange(CAP, dtype=jnp.int32)
    placing = (slot_index[None, :] == columns[:, None]) & (routed[None, :] > 0)
    place_half = placing.astype(jnp.bfloat16)
    place_full = placing.astype(jnp.float32)
    outgoing = jnp.dot(place_half, tokens, preferred_element_type=jnp.float32).astype(jnp.bfloat16)
    weights_f = weight_q.astype(jnp.float32)
    shares = weights_f / jnp.sum(weights_f, axis=1, keepdims=True)
    token_gate = jnp.sum(hits.astype(jnp.float32) * shares, axis=1)
    slot_gate = jnp.dot(place_full, token_gate, precision=lax.Precision.HIGHEST)
    depth = w_gate.shape[1]
    half = outgoing.reshape(CAP, owners, depth).transpose(1, 0, 2)
    piece = lax.all_to_all(half, "gy", split_axis=0, concat_axis=0, tiled=True)
    piece = piece.reshape(owners * CAP, depth)
    gate = jnp.dot(piece, w_gate[0], preferred_element_type=jnp.float32)
    upper = jnp.dot(piece, w_up[0], preferred_element_type=jnp.float32)
    both = lax.psum_scatter(jnp.stack([gate, upper]), "gy", scatter_dimension=2, tiled=True)
    hidden = (jax.nn.silu(both[0]) * both[1]).astype(jnp.bfloat16)
    down_local = w_down[0]
    partial_value = jnp.dot(
        lax.all_gather(hidden, "gy", axis=1, tiled=True),
        down_local,
        preferred_element_type=jnp.float32,
    )
    portion = CAP // width_z
    column_width = partial_value.shape[1]
    blocks = partial_value.reshape(owners, width_z, portion, column_width)
    narrowed = lax.psum_scatter(blocks, "gz", scatter_dimension=1, tiled=True)
    arrived = lax.all_to_all(narrowed, "gy", split_axis=0, concat_axis=1, tiled=True)
    full = jnp.transpose(arrived[0], (1, 0, 2)).reshape(portion, owners * column_width)
    first = lax.axis_index("gz") * portion
    gate_part = lax.dynamic_slice_in_dim(slot_gate, first, portion, 0)
    place_part = lax.dynamic_slice_in_dim(place_full, first, portion, 0)
    weighted = gate_part[:, None] * full
    contribution = jnp.dot(place_part.T, weighted, precision=lax.Precision.HIGHEST)
    result = lax.psum_scatter(contribution, ("gx", "gz"), scatter_dimension=1, tiled=True)
    return result.astype(jnp.bfloat16)


def kernel(sizes, tok_hbm, route_hbm, wq_hbm, wg_hbm, wu_hbm, wd_hbm, out_ref,
           tok, route, wq, gbuf, ubuf, dbuf_a, dbuf_b, xb, xsend, xs, part, precv,
           hid, late, acc, sbuf, rbuf, sem_in, sem_g, sem_u, sem_a, sem_b, stage,
           tok_ss, tok_rs, ex_ss, ex_rs, hid_ss, hid_rs, out_ss, out_rs):
    nx, ny, nz = sizes
    gx, gy, gz = lax.axis_index("gx"), lax.axis_index("gy"), lax.axis_index("gz")
    other = 1 - gy
    depth, ffl = wg_hbm.shape[1], wg_hbm.shape[2]
    cn = ffl // STEPS
    hw = cn // ny
    width = wd_hbm.shape[2]
    nb = nx * nz // ny
    bw = width // nb
    token_rows = tok.shape[0]
    kb = EARLY * cn
    partner = (gx, other, gz)

    def pair(j):
        slot = lax.rem(j, RING)
        cols = pl.ds(pl.multiple_of(j * cn, cn), cn)
        return (pltpu.make_async_copy(wg_hbm.at[0, :, cols], gbuf.at[slot], sem_g.at[slot]),
                pltpu.make_async_copy(wu_hbm.at[0, :, cols], ubuf.at[slot], sem_u.at[slot]))

    def down_a(j):
        rows = pl.ds(pl.multiple_of(j * cn, cn), cn)
        return pltpu.make_async_copy(wd_hbm.at[0, rows, :], dbuf_a.at[j], sem_a.at[j])

    per = nb // nz

    def block_of(i):
        z = jnp.where(gz < nz // 2, nz - 1 - i // per, i // per)
        return lax.rem(i, per) * nz + z, lax.rem(i, per), z

    def down_b(i):
        b, _, _ = block_of(i)
        cols = pl.ds(pl.multiple_of(b * bw, 128), bw)
        return pltpu.make_async_copy(
            wd_hbm.at[0, kb:, cols],
            dbuf_b.at[i // per, :, pl.ds(pl.multiple_of(lax.rem(i, per) * bw, 128), bw)],
            sem_b.at[i])

    ins = [pltpu.make_async_copy(tok_hbm, tok, sem_in.at[0]),
           pltpu.make_async_copy(route_hbm, route, sem_in.at[1]),
           pltpu.make_async_copy(wq_hbm, wq, sem_in.at[2])]
    for c in ins:
        c.start()
    for j in range(1):
        for c in pair(j):
            c.start()

    line_count = (gz > 0).astype(jnp.int32) + (gz < nz - 1).astype(jnp.int32)

    def signal_line(sem):
        @pl.when(gz > 0)
        def _():
            pl.semaphore_signal(sem, inc=1, device_id=(gx, gy, gz - 1), device_id_type=MESH)

        @pl.when(gz < nz - 1)
        def _():
            pl.semaphore_signal(sem, inc=1, device_id=(gx, gy, gz + 1), device_id_type=MESH)

    barrier = pltpu.get_barrier_semaphore()
    pl.semaphore_signal(barrier, inc=1, device_id=partner, device_id_type=MESH)
    for d in range(1, nx):
        pl.semaphore_signal(barrier, inc=1, device_id=(lax.rem(gx + d, nx), gy, gz), device_id_type=MESH)
    signal_line(barrier)

    for c in ins:
        c.wait()
    for j in range(1, RING):
        for c in pair(j):
            c.start()

    lane_t = lax.broadcasted_iota(jnp.int32, (token_rows, token_rows), 1)
    sub_t = lax.broadcasted_iota(jnp.int32, (token_rows, token_rows), 0)
    eye = (lane_t == sub_t).astype(F32)
    upto = (lane_t <= sub_t).astype(F32)
    since = (sub_t <= lane_t).astype(F32)
    r0, r1 = route[0:1, :], route[1:2, :]
    shift = gy.astype(F32) * (PIECE - CAP)

    def hit_row(e):
        return ((r0 == e) | (r1 == e)).astype(F32)

    def row_of(slot):
        return jnp.where(slot < LOW, slot, slot + shift)

    hr = hit_row(gx)
    hc = jnp.sum(eye * hr, axis=1, keepdims=True)
    slot_row = row_of(jnp.sum(since * hc, axis=0, keepdims=True) - 1.0)
    rows_sub = lax.broadcasted_iota(jnp.int32, (PIECE, token_rows), 0).astype(F32)
    place = ((slot_row == rows_sub) & (hr > 0.0)).astype(F32).astype(BF16)

    thirds = 3
    span = depth // thirds
    for q in range(thirds):
        theirs = pl.ds(pl.multiple_of(other * depth + q * span, 128), span)
        xsend[q] = jnp.dot(place, tok[:, theirs], preferred_element_type=F32).astype(BF16)

    pl.semaphore_wait(barrier, (nx - 1) + (ny - 1) + line_count)
    tok_copies = [pltpu.make_async_remote_copy(
        src_ref=xsend.at[q], dst_ref=xb.at[gy, q], send_sem=tok_ss.at[q], recv_sem=tok_rs.at[q],
        device_id=partner, device_id_type=MESH) for q in range(thirds)]
    for c in tok_copies:
        c.start()
    pl.semaphore_signal(stage.at[0], inc=1, device_id=partner, device_id_type=MESH)

    for q in range(thirds):
        ours = pl.ds(pl.multiple_of(gy * depth + q * span, 128), span)
        xb[gy, q] = jnp.dot(place, tok[:, ours], preferred_element_type=F32).astype(BF16)
    acc[...] = jnp.zeros_like(acc)

    w0, w1 = wq[0:1, :].astype(F32), wq[1:2, :].astype(F32)
    total = w0 + w1
    s0, s1 = w0 / total, w1 / total
    spreads = []
    rows_lane = lax.broadcasted_iota(jnp.int32, (token_rows, PIECE), 1).astype(F32)
    for e in range(nx):
        h = hit_row(e)
        g = jnp.where(r0 == e, s0, 0.0) + jnp.where(r1 == e, s1, 0.0)
        slot_col = row_of(jnp.sum(upto * h, axis=1, keepdims=True) - 1.0)
        gate_col = jnp.sum(eye * g, axis=1, keepdims=True)
        hit_col = jnp.sum(eye * h, axis=1, keepdims=True)
        spreads.append(jnp.where((slot_col == rows_lane) & (hit_col > 0.0), gate_col, 0.0))

    def exchange(j):
        return pltpu.make_async_remote_copy(
            src_ref=part.at[j, other], dst_ref=precv.at[j], send_sem=ex_ss.at[j],
            recv_sem=ex_rs.at[j], device_id=partner, device_id_type=MESH)

    def share(j):
        return pltpu.make_async_remote_copy(
            src_ref=hid.at[j, gy], dst_ref=hid.at[j, gy], send_sem=hid_ss.at[j],
            recv_sem=hid_rs.at[j], device_id=partner, device_id_type=MESH)

    def finish(j):
        exchange(j).wait_recv()
        g = part[j, gy, 0] + precv[j, 0]
        u = part[j, gy, 1] + precv[j, 1]
        hid[j, gy] = (g * jax.nn.sigmoid(g) * u).astype(BF16)
        share(j).start()

    def fetch_next(j):
        @pl.when(j + RING < STEPS)
        def _():
            for c in pair(j + RING):
                c.start()

        t = j + RING - STEPS

        @pl.when((t >= 0) & (t < EARLY // 2))
        def _():
            down_a(2 * t).start()
            down_a(2 * t + 1).start()

        @pl.when(t == EARLY // 2)
        def _():
            for i in range(nb):
                down_b(i).start()

    def hand_over(j, g, u):
        for h in range(ny):
            part[j, h, 0] = g[:, h * hw:(h + 1) * hw]
            part[j, h, 1] = u[:, h * hw:(h + 1) * hw]
        exchange(j).start()
        fetch_next(j)

    for c in pair(0):
        c.wait()
    g = u = jnp.zeros((ROWS, cn), F32)
    for q in range(thirds):
        cols = slice(q * span, (q + 1) * span)
        tok_copies[q].wait()
        x0, x1 = xb[0, q].astype(F32), xb[1, q].astype(F32)
        x = jnp.concatenate([x0[:LOW], x1[:LOW], x0[LOW:] + x1[LOW:]], axis=0).astype(BF16)
        xs[:, cols] = x
        g = g + jnp.dot(x, gbuf[0, cols, :], preferred_element_type=F32)
        u = u + jnp.dot(x, ubuf[0, cols, :], preferred_element_type=F32)
    hand_over(0, g, u)

    def project(j, carry):
        @pl.when(j == 1)
        def _():
            pl.semaphore_wait(stage.at[0], ny - 1)

        @pl.when((j > 1) & (j <= nz))
        def _():
            pl.semaphore_wait(stage.at[j - 1], line_count)

        @pl.when(j < nz)
        def _():
            signal_line(stage.at[j])

        for c in pair(j):
            c.wait()
        slot = lax.rem(j, RING)
        g = jnp.dot(xs[...], gbuf[slot], preferred_element_type=F32)
        u = jnp.dot(xs[...], ubuf[slot], preferred_element_type=F32)
        hand_over(j, g, u)

        @pl.when(j >= LAG)
        def _():
            finish(j - LAG)
        return carry

    lax.fori_loop(1, STEPS, project, 0)

    nsub = 4
    sw = width // nsub

    def first_part(j, carry):
        share(j).wait_recv()
        down_a(j).wait()
        for q in range(nsub):
            cols = slice(q * sw, (q + 1) * sw)
            y = acc[:, cols]
            for h in range(ny):
                y = y + jnp.dot(hid[j, h], dbuf_a[j, h * hw:(h + 1) * hw, cols],
                                preferred_element_type=F32)
            acc[:, cols] = y

        @pl.when(j < LAG)
        def _():
            finish(STEPS - LAG + j)
        return carry

    lax.fori_loop(0, EARLY, first_part, 0)
    for j in range(EARLY, STEPS):
        share(j).wait_recv()
        for h in range(ny):
            start = (j - EARLY) * cn + h * hw
            late[:, start:start + hw] = hid[j, h]

    def out_copy(i, o):
        _, c, z = block_of(i)
        here = gx * nz + gz
        return pltpu.make_async_remote_copy(
            src_ref=sbuf.at[i, o], dst_ref=rbuf.at[here], send_sem=out_ss.at[i, o],
            recv_sem=out_rs.at[here], device_id=(gy * per + c, o, z), device_id_type=MESH)

    def to_self(i, o):
        _, c, z = block_of(i)
        return (gy * per + c == gx) & (o == gy) & (z == gz)

    def second_part(k, carry):
        for c in range(per):
            down_b(k * per + c).wait()
        y = jnp.dot(late[...], dbuf_b[k], preferred_element_type=F32)
        for c in range(per):
            i = k * per + c
            b, _, _ = block_of(i)
            yc = acc[:, pl.ds(pl.multiple_of(b * bw, 128), bw)] + y[:, c * bw:(c + 1) * bw]
            for o in range(ny):
                sent = jnp.concatenate([yc[o * LOW:(o + 1) * LOW], yc[ny * LOW:]], axis=0).astype(BF16)
                sbuf[i, o] = sent

                @pl.when(to_self(i, o))
                def _():
                    rbuf[gx * nz + gz] = sent

                @pl.when(jnp.logical_not(to_self(i, o)))
                def _():
                    out_copy(i, o).start()
        return carry

    lax.fori_loop(0, nz, second_part, 0)

    src_y = (gx * nz + gz) // nb
    for e in range(nx):
        for z in range(nz):
            @pl.when(jnp.logical_not((e == gx) & (src_y == gy) & (z == gz)))
            def _():
                pltpu.make_async_remote_copy(
                    src_ref=sbuf.at[0, 0], dst_ref=rbuf.at[e * nz + z], send_sem=out_ss.at[0, 0],
                    recv_sem=out_rs.at[e * nz + z], device_id=(e, src_y, z),
                    device_id_type=MESH).wait_recv()
    sums = []
    for e in range(nx):
        s = rbuf[e * nz].astype(F32)
        for z in range(1, nz):
            s = s + rbuf[e * nz + z].astype(F32)
        sums.append(jnp.dot(spreads[e], s, precision=lax.Precision.HIGHEST,
                            preferred_element_type=F32))
    out_ref[...] = functools.reduce(lambda a, b: a + b, sums).astype(out_ref.dtype)

    def drain(j, carry):
        exchange(j).wait_send()
        share(j).wait_send()
        return carry

    lax.fori_loop(0, STEPS, drain, 0)

    def drain_out(i, carry):
        for o in range(ny):
            @pl.when(jnp.logical_not(to_self(i, o)))
            def _():
                out_copy(i, o).wait_send()
        return carry

    lax.fori_loop(0, nb, drain_out, 0)


def fused(sizes, tokens, route, weight_q, w_gate, w_up, w_down):
    nx, ny, nz = sizes
    depth, ffl = w_gate.shape[1], w_gate.shape[2]
    width = w_down.shape[2]
    cn = ffl // STEPS
    hw = cn // ny
    nb = nx * nz // ny
    bw = width // nb
    rest = ffl - EARLY * cn
    dma = pltpu.SemaphoreType.DMA
    hbm = pl.BlockSpec(memory_space=pl.ANY)
    return pl.pallas_call(
        functools.partial(kernel, sizes),
        out_shape=jax.ShapeDtypeStruct((tokens.shape[0], bw), BF16),
        in_specs=[hbm] * 6,
        out_specs=pl.BlockSpec(memory_space=pltpu.VMEM),
        scratch_shapes=[
            pltpu.VMEM(tokens.shape, BF16),
            pltpu.VMEM(route.shape[::-1], jnp.int32),
            pltpu.VMEM(route.shape[::-1], jnp.int32),
            pltpu.VMEM((RING, depth, cn), BF16),
            pltpu.VMEM((RING, depth, cn), BF16),
            pltpu.VMEM((EARLY, cn, width), BF16),
            pltpu.VMEM((nz, rest, nb // nz * bw), BF16),
            pltpu.VMEM((ny, 3, PIECE, depth // 3), BF16),
            pltpu.VMEM((3, PIECE, depth // 3), BF16),
            pltpu.VMEM((ROWS, depth), BF16),
            pltpu.VMEM((STEPS, ny, 2, ROWS, hw), F32),
            pltpu.VMEM((STEPS, 2, ROWS, hw), F32),
            pltpu.VMEM((STEPS, ny, ROWS, hw), BF16),
            pltpu.VMEM((ROWS, rest), BF16),
            pltpu.VMEM((ROWS, width), F32),
            pltpu.VMEM((nb, ny, PIECE, bw), BF16),
            pltpu.VMEM((nx * nz, PIECE, bw), BF16),
            dma((3,)), dma((RING,)), dma((RING,)), dma((EARLY,)), dma((nb,)),
            pltpu.SemaphoreType.REGULAR((nz,)),
            dma((3,)), dma((3,)), dma((STEPS,)), dma((STEPS,)), dma((STEPS,)), dma((STEPS,)),
            dma((nb, ny)), dma((nx * nz,)),
        ],
        compiler_params=pltpu.CompilerParams(
            collective_id=0, has_side_effects=True, vmem_limit_bytes=67043328),
        name="routed_ffn",
    )(tokens, route.T, weight_q.T, w_gate, w_up, w_down)


def solution(mesh):
    in_specs = (
        P("gy", None),
        P("gy", None),
        P("gy", None),
        P("gx", "gy", "gz"),
        P("gx", "gy", "gz"),
        P("gx", "gz", "gy"),
    )
    out_specs = P("gy", ("gx", "gz"))
    sizes = tuple(mesh.shape[name] for name in ("gx", "gy", "gz"))
    body = functools.partial(fused, sizes) if sizes[1] == 2 else plain
    return jax.shard_map(
        body, mesh=mesh, in_specs=in_specs, out_specs=out_specs, check_vma=False
    )
```

```python
import functools

import jax
import jax.numpy as jnp
from jax import lax
from jax.experimental import pallas as pl
from jax.experimental.pallas import tpu as pltpu
from jax.sharding import PartitionSpec as P

CAP = 12
LOW = 8
PIECE = 16
ROWS = 24
STEPS = 8
EARLY = 4
DIRECT = 2
RING = 5
LAG = 3
MESH = pl.DeviceIdType.MESH
F32, BF16 = jnp.float32, jnp.bfloat16


def plain(tokens, route, weight_q, w_gate, w_up, w_down):
    expert = lax.axis_index("gx")
    width_z = lax.axis_size("gz")
    owners = lax.axis_size("gy")
    hits = (route == expert).astype(jnp.int32)
    routed = jnp.sum(hits, axis=1)
    slot_index = jnp.cumsum(routed) - 1
    columns = jnp.arange(CAP, dtype=jnp.int32)
    placing = (slot_index[None, :] == columns[:, None]) & (routed[None, :] > 0)
    place_half = placing.astype(jnp.bfloat16)
    place_full = placing.astype(jnp.float32)
    outgoing = jnp.dot(place_half, tokens, preferred_element_type=jnp.float32).astype(jnp.bfloat16)
    weights_f = weight_q.astype(jnp.float32)
    shares = weights_f / jnp.sum(weights_f, axis=1, keepdims=True)
    token_gate = jnp.sum(hits.astype(jnp.float32) * shares, axis=1)
    slot_gate = jnp.dot(place_full, token_gate, precision=lax.Precision.HIGHEST)
    depth = w_gate.shape[1]
    half = outgoing.reshape(CAP, owners, depth).transpose(1, 0, 2)
    piece = lax.all_to_all(half, "gy", split_axis=0, concat_axis=0, tiled=True)
    piece = piece.reshape(owners * CAP, depth)
    gate = jnp.dot(piece, w_gate[0], preferred_element_type=jnp.float32)
    upper = jnp.dot(piece, w_up[0], preferred_element_type=jnp.float32)
    both = lax.psum_scatter(jnp.stack([gate, upper]), "gy", scatter_dimension=2, tiled=True)
    hidden = (jax.nn.silu(both[0]) * both[1]).astype(jnp.bfloat16)
    down_local = w_down[0]
    partial_value = jnp.dot(
        lax.all_gather(hidden, "gy", axis=1, tiled=True),
        down_local,
        preferred_element_type=jnp.float32,
    )
    portion = CAP // width_z
    column_width = partial_value.shape[1]
    blocks = partial_value.reshape(owners, width_z, portion, column_width)
    narrowed = lax.psum_scatter(blocks, "gz", scatter_dimension=1, tiled=True)
    arrived = lax.all_to_all(narrowed, "gy", split_axis=0, concat_axis=1, tiled=True)
    full = jnp.transpose(arrived[0], (1, 0, 2)).reshape(portion, owners * column_width)
    first = lax.axis_index("gz") * portion
    gate_part = lax.dynamic_slice_in_dim(slot_gate, first, portion, 0)
    place_part = lax.dynamic_slice_in_dim(place_full, first, portion, 0)
    weighted = gate_part[:, None] * full
    contribution = jnp.dot(place_part.T, weighted, precision=lax.Precision.HIGHEST)
    result = lax.psum_scatter(contribution, ("gx", "gz"), scatter_dimension=1, tiled=True)
    return result.astype(jnp.bfloat16)


def kernel(sizes, tok_hbm, route_hbm, wq_hbm, wg_hbm, wu_hbm, wd_hbm, out_ref,
           tok, route, wq, gbuf, ubuf, dbuf_a, dbuf_b, xb, xsend, xs, part, precv,
           whole, wrecv, hid, late, acc, sbuf, rbuf, sem_in, sem_g, sem_u, sem_a, sem_b, stage,
           tok_ss, tok_rs, cr_ss, cr_rs, ex_ss, ex_rs, hid_ss, hid_rs, out_ss, out_rs):
    nx, ny, nz = sizes
    gx, gy, gz = lax.axis_index("gx"), lax.axis_index("gy"), lax.axis_index("gz")
    other = 1 - gy
    depth, ffl = wg_hbm.shape[1], wg_hbm.shape[2]
    cn = ffl // STEPS
    hw = cn // ny
    width = wd_hbm.shape[2]
    nb = nx * nz // ny
    bw = width // nb
    token_rows = tok.shape[0]
    kb = EARLY * cn
    partner = (gx, other, gz)

    def pair(j):
        slot = lax.rem(j, RING)
        cols = pl.ds(pl.multiple_of(j * cn, cn), cn)
        return (pltpu.make_async_copy(wg_hbm.at[0, :, cols], gbuf.at[slot], sem_g.at[slot]),
                pltpu.make_async_copy(wu_hbm.at[0, :, cols], ubuf.at[slot], sem_u.at[slot]))

    def down_a(j):
        rows = pl.ds(pl.multiple_of(j * cn, cn), cn)
        return pltpu.make_async_copy(wd_hbm.at[0, rows, :], dbuf_a.at[j], sem_a.at[j])

    per = nb // nz

    def block_of(i):
        z = jnp.where(gz < nz // 2, nz - 1 - i // per, i // per)
        return lax.rem(i, per) * nz + z, lax.rem(i, per), z

    def down_b(i):
        b, _, _ = block_of(i)
        cols = pl.ds(pl.multiple_of(b * bw, 128), bw)
        return pltpu.make_async_copy(
            wd_hbm.at[0, kb:, cols],
            dbuf_b.at[i // per, :, pl.ds(pl.multiple_of(lax.rem(i, per) * bw, 128), bw)],
            sem_b.at[i])

    ins = [pltpu.make_async_copy(tok_hbm, tok, sem_in.at[0]),
           pltpu.make_async_copy(route_hbm, route, sem_in.at[1]),
           pltpu.make_async_copy(wq_hbm, wq, sem_in.at[2])]
    for c in ins:
        c.start()
    for j in range(1):
        for c in pair(j):
            c.start()

    line_count = (gz > 0).astype(jnp.int32) + (gz < nz - 1).astype(jnp.int32)

    def signal_line(sem):
        @pl.when(gz > 0)
        def _():
            pl.semaphore_signal(sem, inc=1, device_id=(gx, gy, gz - 1), device_id_type=MESH)

        @pl.when(gz < nz - 1)
        def _():
            pl.semaphore_signal(sem, inc=1, device_id=(gx, gy, gz + 1), device_id_type=MESH)

    barrier = pltpu.get_barrier_semaphore()
    pl.semaphore_signal(barrier, inc=1, device_id=partner, device_id_type=MESH)
    for d in range(1, nx):
        pl.semaphore_signal(barrier, inc=1, device_id=(lax.rem(gx + d, nx), gy, gz), device_id_type=MESH)
    signal_line(barrier)

    for c in ins:
        c.wait()
    for j in range(1, RING):
        for c in pair(j):
            c.start()

    lane_t = lax.broadcasted_iota(jnp.int32, (token_rows, token_rows), 1)
    sub_t = lax.broadcasted_iota(jnp.int32, (token_rows, token_rows), 0)
    eye = (lane_t == sub_t).astype(F32)
    upto = (lane_t <= sub_t).astype(F32)
    since = (sub_t <= lane_t).astype(F32)
    r0, r1 = route[0:1, :], route[1:2, :]
    shift = gy.astype(F32) * (PIECE - CAP)

    def hit_row(e):
        return ((r0 == e) | (r1 == e)).astype(F32)

    def row_of(slot):
        return jnp.where(slot < LOW, slot, slot + shift)

    hr = hit_row(gx)
    hc = jnp.sum(eye * hr, axis=1, keepdims=True)
    slot_row = row_of(jnp.sum(since * hc, axis=0, keepdims=True) - 1.0)
    rows_sub = lax.broadcasted_iota(jnp.int32, (PIECE, token_rows), 0).astype(F32)
    place = ((slot_row == rows_sub) & (hr > 0.0)).astype(F32).astype(BF16)

    thirds = 3
    span = depth // thirds
    for q in range(thirds):
        theirs = pl.ds(pl.multiple_of(other * depth + q * span, 128), span)
        xsend[q] = jnp.dot(place, tok[:, theirs], preferred_element_type=F32).astype(BF16)

    pl.semaphore_wait(barrier, (nx - 1) + (ny - 1) + line_count)
    tok_copies = [pltpu.make_async_remote_copy(
        src_ref=xsend.at[q], dst_ref=xb.at[gy, q], send_sem=tok_ss.at[q], recv_sem=tok_rs.at[q],
        device_id=partner, device_id_type=MESH) for q in range(thirds)]
    for c in tok_copies:
        c.start()
    pl.semaphore_signal(stage.at[0], inc=1, device_id=partner, device_id_type=MESH)

    for q in range(thirds):
        ours = pl.ds(pl.multiple_of(gy * depth + q * span, 128), span)
        xb[gy, q] = jnp.dot(place, tok[:, ours], preferred_element_type=F32).astype(BF16)
    acc[...] = jnp.zeros_like(acc)

    w0, w1 = wq[0:1, :].astype(F32), wq[1:2, :].astype(F32)
    total = w0 + w1
    s0, s1 = w0 / total, w1 / total
    spreads = []
    rows_lane = lax.broadcasted_iota(jnp.int32, (token_rows, PIECE), 1).astype(F32)
    for e in range(nx):
        h = hit_row(e)
        g = jnp.where(r0 == e, s0, 0.0) + jnp.where(r1 == e, s1, 0.0)
        slot_col = row_of(jnp.sum(upto * h, axis=1, keepdims=True) - 1.0)
        gate_col = jnp.sum(eye * g, axis=1, keepdims=True)
        hit_col = jnp.sum(eye * h, axis=1, keepdims=True)
        spreads.append(jnp.where((slot_col == rows_lane) & (hit_col > 0.0), gate_col, 0.0))

    def exchange(j):
        return pltpu.make_async_remote_copy(
            src_ref=part.at[j, other], dst_ref=precv.at[j], send_sem=ex_ss.at[j],
            recv_sem=ex_rs.at[j], device_id=partner, device_id_type=MESH)

    def share(j):
        return pltpu.make_async_remote_copy(
            src_ref=hid.at[j, gy], dst_ref=hid.at[j, gy], send_sem=hid_ss.at[j],
            recv_sem=hid_rs.at[j], device_id=partner, device_id_type=MESH)

    def finish(j):
        exchange(j).wait_recv()
        g = part[j, gy, 0] + precv[j, 0]
        u = part[j, gy, 1] + precv[j, 1]
        hid[j, gy] = (g * jax.nn.sigmoid(g) * u).astype(BF16)
        share(j).start()

    def fetch_next(j):
        @pl.when(j + RING < STEPS)
        def _():
            for c in pair(j + RING):
                c.start()

        @pl.when(j == STEPS - RING + 1)
        def _():
            for t in range(EARLY - 2):
                down_a(t).start()

        @pl.when(j == STEPS - RING + 2)
        def _():
            down_a(EARLY - 2).start()

        @pl.when(j == STEPS - RING + 3)
        def _():
            down_a(EARLY - 1).start()

    def hand_over(j, g, u):
        for h in range(ny):
            part[j, h, 0] = g[:, h * hw:(h + 1) * hw]
            part[j, h, 1] = u[:, h * hw:(h + 1) * hw]

    for c in pair(0):
        c.wait()
    g = u = jnp.zeros((ROWS, cn), F32)
    for q in range(thirds):
        cols = slice(q * span, (q + 1) * span)
        tok_copies[q].wait()
        x0, x1 = xb[0, q].astype(F32), xb[1, q].astype(F32)
        x = jnp.concatenate([x0[:LOW], x1[:LOW], x0[LOW:] + x1[LOW:]], axis=0).astype(BF16)
        xs[:, cols] = x
        g = g + jnp.dot(x, gbuf[0, cols, :], preferred_element_type=F32)
        u = u + jnp.dot(x, ubuf[0, cols, :], preferred_element_type=F32)
    hand_over(0, g, u)
    exchange(0).start()
    fetch_next(0)

    def multiply(j):
        for c in pair(j):
            c.wait()
        slot = lax.rem(j, RING)
        g = jnp.dot(xs[...], gbuf[slot], preferred_element_type=F32)
        u = jnp.dot(xs[...], ubuf[slot], preferred_element_type=F32)
        hand_over(j, g, u)
        return g, u

    def cross(d):
        return pltpu.make_async_remote_copy(
            src_ref=whole.at[d], dst_ref=wrecv.at[d], send_sem=cr_ss.at[d],
            recv_sem=cr_rs.at[d], device_id=partner, device_id_type=MESH)

    def project(j, carry):
        @pl.when(j == 1)
        def _():
            pl.semaphore_wait(stage.at[0], ny - 1)

        @pl.when((j > 1) & (j <= nz))
        def _():
            pl.semaphore_wait(stage.at[j - 1], line_count)

        @pl.when(j < nz)
        def _():
            signal_line(stage.at[j])

        multiply(j)
        exchange(j).start()
        fetch_next(j)

        @pl.when(j >= LAG)
        def _():
            finish(j - LAG)
        return carry

    def project_last(j, carry):
        g, u = multiply(j)
        d = j - (STEPS - DIRECT)
        whole[d] = jnp.concatenate([g, u], axis=0).astype(BF16)
        cross(d).start()
        fetch_next(j)
        finish(j - LAG)
        return carry

    lax.fori_loop(1, STEPS - DIRECT, project, 0)
    lax.fori_loop(STEPS - DIRECT, STEPS, project_last, 0)

    nsub = 4
    sw = width // nsub

    def fetch_blocks(k):
        for c in range(per):
            down_b(k * per + c).start()

    def first_part(j, carry):
        @pl.when(j < nz)
        def _():
            fetch_blocks(j)

        share(j).wait_recv()
        down_a(j).wait()
        for q in range(nsub):
            cols = slice(q * sw, (q + 1) * sw)
            y = acc[:, cols]
            for h in range(ny):
                y = y + jnp.dot(hid[j, h], dbuf_a[j, h * hw:(h + 1) * hw, cols],
                                preferred_element_type=F32)
            acc[:, cols] = y

        @pl.when(j < LAG - DIRECT)
        def _():
            finish(STEPS - LAG + j)
        return carry

    lax.fori_loop(0, EARLY, first_part, 0)
    for k in range(EARLY, nz):
        fetch_blocks(k)
    for j in range(EARLY, STEPS):
        d = j - (STEPS - DIRECT)
        if d < 0:
            share(j).wait_recv()
        else:
            cross(d).wait_recv()
        for h in range(ny):
            start = (j - EARLY) * cn + h * hw
            if d < 0:
                late[:, start:start + hw] = hid[j, h]
            else:
                theirs = wrecv[d, :, h * hw:(h + 1) * hw].astype(F32)
                g = part[j, h, 0] + theirs[:ROWS]
                u = part[j, h, 1] + theirs[ROWS:]
                late[:, start:start + hw] = (g * jax.nn.sigmoid(g) * u).astype(BF16)

    def out_copy(i, o):
        _, c, z = block_of(i)
        here = gx * nz + gz
        return pltpu.make_async_remote_copy(
            src_ref=sbuf.at[i, o], dst_ref=rbuf.at[here], send_sem=out_ss.at[i, o],
            recv_sem=out_rs.at[here], device_id=(gy * per + c, o, z), device_id_type=MESH)

    def to_self(i, o):
        _, c, z = block_of(i)
        return (gy * per + c == gx) & (o == gy) & (z == gz)

    def second_part(k, carry):
        for c in range(per):
            down_b(k * per + c).wait()
        y = jnp.dot(late[...], dbuf_b[k], preferred_element_type=F32)
        for c in range(per):
            i = k * per + c
            b, _, _ = block_of(i)
            yc = acc[:, pl.ds(pl.multiple_of(b * bw, 128), bw)] + y[:, c * bw:(c + 1) * bw]
            for o in range(ny):
                sent = jnp.concatenate([yc[o * LOW:(o + 1) * LOW], yc[ny * LOW:]], axis=0).astype(BF16)
                sbuf[i, o] = sent

                @pl.when(to_self(i, o))
                def _():
                    rbuf[gx * nz + gz] = sent

                @pl.when(jnp.logical_not(to_self(i, o)))
                def _():
                    out_copy(i, o).start()
        return carry

    lax.fori_loop(0, nz, second_part, 0)

    src_y = (gx * nz + gz) // nb
    for e in range(nx):
        for z in range(nz):
            @pl.when(jnp.logical_not((e == gx) & (src_y == gy) & (z == gz)))
            def _():
                pltpu.make_async_remote_copy(
                    src_ref=sbuf.at[0, 0], dst_ref=rbuf.at[e * nz + z], send_sem=out_ss.at[0, 0],
                    recv_sem=out_rs.at[e * nz + z], device_id=(e, src_y, z),
                    device_id_type=MESH).wait_recv()
    sums = []
    for e in range(nx):
        s = rbuf[e * nz].astype(F32)
        for z in range(1, nz):
            s = s + rbuf[e * nz + z].astype(F32)
        sums.append(jnp.dot(spreads[e], s, precision=lax.Precision.HIGHEST,
                            preferred_element_type=F32))
    out_ref[...] = functools.reduce(lambda a, b: a + b, sums).astype(out_ref.dtype)

    def drain(j, carry):
        exchange(j).wait_send()
        share(j).wait_send()
        return carry

    lax.fori_loop(0, STEPS - DIRECT, drain, 0)
    for d in range(DIRECT):
        cross(d).wait_send()

    def drain_out(i, carry):
        for o in range(ny):
            @pl.when(jnp.logical_not(to_self(i, o)))
            def _():
                out_copy(i, o).wait_send()
        return carry

    lax.fori_loop(0, nb, drain_out, 0)


def fused(sizes, tokens, route, weight_q, w_gate, w_up, w_down):
    nx, ny, nz = sizes
    depth, ffl = w_gate.shape[1], w_gate.shape[2]
    width = w_down.shape[2]
    cn = ffl // STEPS
    hw = cn // ny
    nb = nx * nz // ny
    bw = width // nb
    rest = ffl - EARLY * cn
    dma = pltpu.SemaphoreType.DMA
    hbm = pl.BlockSpec(memory_space=pl.ANY)
    return pl.pallas_call(
        functools.partial(kernel, sizes),
        out_shape=jax.ShapeDtypeStruct((tokens.shape[0], bw), BF16),
        in_specs=[hbm] * 6,
        out_specs=pl.BlockSpec(memory_space=pltpu.VMEM),
        scratch_shapes=[
            pltpu.VMEM(tokens.shape, BF16),
            pltpu.VMEM(route.shape[::-1], jnp.int32),
            pltpu.VMEM(route.shape[::-1], jnp.int32),
            pltpu.VMEM((RING, depth, cn), BF16),
            pltpu.VMEM((RING, depth, cn), BF16),
            pltpu.VMEM((EARLY, cn, width), BF16),
            pltpu.VMEM((nz, rest, nb // nz * bw), BF16),
            pltpu.VMEM((ny, 3, PIECE, depth // 3), BF16),
            pltpu.VMEM((3, PIECE, depth // 3), BF16),
            pltpu.VMEM((ROWS, depth), BF16),
            pltpu.VMEM((STEPS, ny, 2, ROWS, hw), F32),
            pltpu.VMEM((STEPS - DIRECT, 2, ROWS, hw), F32),
            pltpu.VMEM((DIRECT, 2 * ROWS, cn), BF16),
            pltpu.VMEM((DIRECT, 2 * ROWS, cn), BF16),
            pltpu.VMEM((STEPS - DIRECT, ny, ROWS, hw), BF16),
            pltpu.VMEM((ROWS, rest), BF16),
            pltpu.VMEM((ROWS, width), F32),
            pltpu.VMEM((nb, ny, PIECE, bw), BF16),
            pltpu.VMEM((nx * nz, PIECE, bw), BF16),
            dma((3,)), dma((RING,)), dma((RING,)), dma((EARLY,)), dma((nb,)),
            pltpu.SemaphoreType.REGULAR((nz,)),
            dma((3,)), dma((3,)), dma((DIRECT,)), dma((DIRECT,)),
            *[dma((STEPS - DIRECT,))] * 4,
            dma((nb, ny)), dma((nx * nz,)),
        ],
        compiler_params=pltpu.CompilerParams(
            collective_id=0, has_side_effects=True, vmem_limit_bytes=67043328),
        name="routed_ffn",
    )(tokens, route.T, weight_q.T, w_gate, w_up, w_down)


def solution(mesh):
    in_specs = (
        P("gy", None),
        P("gy", None),
        P("gy", None),
        P("gx", "gy", "gz"),
        P("gx", "gy", "gz"),
        P("gx", "gz", "gy"),
    )
    out_specs = P("gy", ("gx", "gz"))
    sizes = tuple(mesh.shape[name] for name in ("gx", "gy", "gz"))
    body = functools.partial(fused, sizes) if sizes[1] == 2 else plain
    return jax.shard_map(
        body, mesh=mesh, in_specs=in_specs, out_specs=out_specs, check_vma=False
    )
```

```python
import functools

import jax
import jax.numpy as jnp
from jax import lax
from jax.experimental import pallas as pl
from jax.experimental.pallas import tpu as pltpu
from jax.sharding import PartitionSpec as P

CAP = 12
LOW = 8
PIECE = 16
ROWS = 24
STEPS = 8
EARLY = 4
DIRECT = 2
RING = 5
LAG = 2
MESH = pl.DeviceIdType.MESH
F32, BF16 = jnp.float32, jnp.bfloat16


def plain(tokens, route, weight_q, w_gate, w_up, w_down):
    expert = lax.axis_index("gx")
    width_z = lax.axis_size("gz")
    owners = lax.axis_size("gy")
    hits = (route == expert).astype(jnp.int32)
    routed = jnp.sum(hits, axis=1)
    slot_index = jnp.cumsum(routed) - 1
    columns = jnp.arange(CAP, dtype=jnp.int32)
    placing = (slot_index[None, :] == columns[:, None]) & (routed[None, :] > 0)
    place_half = placing.astype(jnp.bfloat16)
    place_full = placing.astype(jnp.float32)
    outgoing = jnp.dot(place_half, tokens, preferred_element_type=jnp.float32).astype(jnp.bfloat16)
    weights_f = weight_q.astype(jnp.float32)
    shares = weights_f / jnp.sum(weights_f, axis=1, keepdims=True)
    token_gate = jnp.sum(hits.astype(jnp.float32) * shares, axis=1)
    slot_gate = jnp.dot(place_full, token_gate, precision=lax.Precision.HIGHEST)
    depth = w_gate.shape[1]
    half = outgoing.reshape(CAP, owners, depth).transpose(1, 0, 2)
    piece = lax.all_to_all(half, "gy", split_axis=0, concat_axis=0, tiled=True)
    piece = piece.reshape(owners * CAP, depth)
    gate = jnp.dot(piece, w_gate[0], preferred_element_type=jnp.float32)
    upper = jnp.dot(piece, w_up[0], preferred_element_type=jnp.float32)
    both = lax.psum_scatter(jnp.stack([gate, upper]), "gy", scatter_dimension=2, tiled=True)
    hidden = (jax.nn.silu(both[0]) * both[1]).astype(jnp.bfloat16)
    down_local = w_down[0]
    partial_value = jnp.dot(
        lax.all_gather(hidden, "gy", axis=1, tiled=True),
        down_local,
        preferred_element_type=jnp.float32,
    )
    portion = CAP // width_z
    column_width = partial_value.shape[1]
    blocks = partial_value.reshape(owners, width_z, portion, column_width)
    narrowed = lax.psum_scatter(blocks, "gz", scatter_dimension=1, tiled=True)
    arrived = lax.all_to_all(narrowed, "gy", split_axis=0, concat_axis=1, tiled=True)
    full = jnp.transpose(arrived[0], (1, 0, 2)).reshape(portion, owners * column_width)
    first = lax.axis_index("gz") * portion
    gate_part = lax.dynamic_slice_in_dim(slot_gate, first, portion, 0)
    place_part = lax.dynamic_slice_in_dim(place_full, first, portion, 0)
    weighted = gate_part[:, None] * full
    contribution = jnp.dot(place_part.T, weighted, precision=lax.Precision.HIGHEST)
    result = lax.psum_scatter(contribution, ("gx", "gz"), scatter_dimension=1, tiled=True)
    return result.astype(jnp.bfloat16)


def kernel(sizes, tok_hbm, route_hbm, wq_hbm, wg_hbm, wu_hbm, wd_hbm, out_ref,
           tok, route, wq, gbuf, ubuf, dbuf_a, dbuf_b, xb, xsend, xs, part, precv,
           whole, wrecv, hid, late, acc, sbuf, rbuf, sem_in, sem_g, sem_u, sem_a, sem_b, stage,
           tok_ss, tok_rs, cr_ss, cr_rs, ex_ss, ex_rs, hid_ss, hid_rs, out_ss, out_rs):
    nx, ny, nz = sizes
    gx, gy, gz = lax.axis_index("gx"), lax.axis_index("gy"), lax.axis_index("gz")
    other = 1 - gy
    depth, ffl = wg_hbm.shape[1], wg_hbm.shape[2]
    cn = ffl // STEPS
    hw = cn // ny
    width = wd_hbm.shape[2]
    nb = nx * nz // ny
    bw = width // nb
    token_rows = tok.shape[0]
    kb = EARLY * cn
    partner = (gx, other, gz)

    def pair(j):
        slot = lax.rem(j, RING)
        cols = pl.ds(pl.multiple_of(j * cn, cn), cn)
        return (pltpu.make_async_copy(wg_hbm.at[0, :, cols], gbuf.at[slot], sem_g.at[slot]),
                pltpu.make_async_copy(wu_hbm.at[0, :, cols], ubuf.at[slot], sem_u.at[slot]))

    def down_a(j):
        rows = pl.ds(pl.multiple_of(j * cn, cn), cn)
        return pltpu.make_async_copy(wd_hbm.at[0, rows, :], dbuf_a.at[j], sem_a.at[j])

    per = nb // nz

    def block_of(i):
        z = jnp.where(gz < nz // 2, nz - 1 - i // per, i // per)
        return lax.rem(i, per) * nz + z, lax.rem(i, per), z

    def down_b(i):
        b, _, _ = block_of(i)
        cols = pl.ds(pl.multiple_of(b * bw, 128), bw)
        return pltpu.make_async_copy(
            wd_hbm.at[0, kb:, cols],
            dbuf_b.at[i // per, :, pl.ds(pl.multiple_of(lax.rem(i, per) * bw, 128), bw)],
            sem_b.at[i])

    ins = [pltpu.make_async_copy(tok_hbm, tok, sem_in.at[0]),
           pltpu.make_async_copy(route_hbm, route, sem_in.at[1]),
           pltpu.make_async_copy(wq_hbm, wq, sem_in.at[2])]
    for c in ins:
        c.start()
    for j in range(1):
        for c in pair(j):
            c.start()

    line_count = (gz > 0).astype(jnp.int32) + (gz < nz - 1).astype(jnp.int32)

    def signal_line(sem):
        @pl.when(gz > 0)
        def _():
            pl.semaphore_signal(sem, inc=1, device_id=(gx, gy, gz - 1), device_id_type=MESH)

        @pl.when(gz < nz - 1)
        def _():
            pl.semaphore_signal(sem, inc=1, device_id=(gx, gy, gz + 1), device_id_type=MESH)

    barrier = pltpu.get_barrier_semaphore()
    pl.semaphore_signal(barrier, inc=1, device_id=partner, device_id_type=MESH)
    for d in range(1, nx):
        pl.semaphore_signal(barrier, inc=1, device_id=(lax.rem(gx + d, nx), gy, gz), device_id_type=MESH)
    signal_line(barrier)

    for c in ins:
        c.wait()
    for j in range(1, RING):
        for c in pair(j):
            c.start()

    lane_t = lax.broadcasted_iota(jnp.int32, (token_rows, token_rows), 1)
    sub_t = lax.broadcasted_iota(jnp.int32, (token_rows, token_rows), 0)
    eye = (lane_t == sub_t).astype(F32)
    upto = (lane_t <= sub_t).astype(F32)
    since = (sub_t <= lane_t).astype(F32)
    r0, r1 = route[0:1, :], route[1:2, :]
    shift = gy.astype(F32) * (PIECE - CAP)

    def hit_row(e):
        return ((r0 == e) | (r1 == e)).astype(F32)

    def row_of(slot):
        return jnp.where(slot < LOW, slot, slot + shift)

    hr = hit_row(gx)
    hc = jnp.sum(eye * hr, axis=1, keepdims=True)
    slot_row = row_of(jnp.sum(since * hc, axis=0, keepdims=True) - 1.0)
    rows_sub = lax.broadcasted_iota(jnp.int32, (PIECE, token_rows), 0).astype(F32)
    place = ((slot_row == rows_sub) & (hr > 0.0)).astype(F32).astype(BF16)

    thirds = 3
    span = depth // thirds
    for q in range(thirds):
        theirs = pl.ds(pl.multiple_of(other * depth + q * span, 128), span)
        xsend[q] = jnp.dot(place, tok[:, theirs], preferred_element_type=F32).astype(BF16)

    pl.semaphore_wait(barrier, (nx - 1) + (ny - 1) + line_count)
    tok_copies = [pltpu.make_async_remote_copy(
        src_ref=xsend.at[q], dst_ref=xb.at[gy, q], send_sem=tok_ss.at[q], recv_sem=tok_rs.at[q],
        device_id=partner, device_id_type=MESH) for q in range(thirds)]
    for c in tok_copies:
        c.start()
    pl.semaphore_signal(stage.at[0], inc=1, device_id=partner, device_id_type=MESH)

    for q in range(thirds):
        ours = pl.ds(pl.multiple_of(gy * depth + q * span, 128), span)
        xb[gy, q] = jnp.dot(place, tok[:, ours], preferred_element_type=F32).astype(BF16)
    acc[...] = jnp.zeros_like(acc)

    w0, w1 = wq[0:1, :].astype(F32), wq[1:2, :].astype(F32)
    total = w0 + w1
    s0, s1 = w0 / total, w1 / total
    spreads = []
    rows_lane = lax.broadcasted_iota(jnp.int32, (token_rows, PIECE), 1).astype(F32)
    for e in range(nx):
        h = hit_row(e)
        g = jnp.where(r0 == e, s0, 0.0) + jnp.where(r1 == e, s1, 0.0)
        slot_col = row_of(jnp.sum(upto * h, axis=1, keepdims=True) - 1.0)
        gate_col = jnp.sum(eye * g, axis=1, keepdims=True)
        hit_col = jnp.sum(eye * h, axis=1, keepdims=True)
        spreads.append(jnp.where((slot_col == rows_lane) & (hit_col > 0.0), gate_col, 0.0))

    def exchange(j):
        return pltpu.make_async_remote_copy(
            src_ref=part.at[j, other], dst_ref=precv.at[j], send_sem=ex_ss.at[j],
            recv_sem=ex_rs.at[j], device_id=partner, device_id_type=MESH)

    def share(j):
        return pltpu.make_async_remote_copy(
            src_ref=hid.at[j, gy], dst_ref=hid.at[j, gy], send_sem=hid_ss.at[j],
            recv_sem=hid_rs.at[j], device_id=partner, device_id_type=MESH)

    def finish(j):
        exchange(j).wait_recv()
        g = part[j, gy, 0] + precv[j, 0]
        u = part[j, gy, 1] + precv[j, 1]
        hid[j, gy] = (g * jax.nn.sigmoid(g) * u).astype(BF16)
        share(j).start()

    def fetch_next(j):
        @pl.when(j + RING < STEPS)
        def _():
            for c in pair(j + RING):
                c.start()

        @pl.when(j == STEPS - RING + 1)
        def _():
            for t in range(EARLY - 2):
                down_a(t).start()

        @pl.when(j == STEPS - RING + 2)
        def _():
            down_a(EARLY - 2).start()

        @pl.when(j == STEPS - RING + 3)
        def _():
            down_a(EARLY - 1).start()

    def hand_over(j, g, u):
        for h in range(ny):
            part[j, h, 0] = g[:, h * hw:(h + 1) * hw]
            part[j, h, 1] = u[:, h * hw:(h + 1) * hw]

    for c in pair(0):
        c.wait()
    g = u = jnp.zeros((ROWS, cn), F32)
    for q in range(thirds):
        cols = slice(q * span, (q + 1) * span)
        tok_copies[q].wait()
        x0, x1 = xb[0, q].astype(F32), xb[1, q].astype(F32)
        x = jnp.concatenate([x0[:LOW], x1[:LOW], x0[LOW:] + x1[LOW:]], axis=0).astype(BF16)
        xs[:, cols] = x
        g = g + jnp.dot(x, gbuf[0, cols, :], preferred_element_type=F32)
        u = u + jnp.dot(x, ubuf[0, cols, :], preferred_element_type=F32)
    hand_over(0, g, u)
    exchange(0).start()
    fetch_next(0)

    def multiply(j):
        for c in pair(j):
            c.wait()
        slot = lax.rem(j, RING)
        g = jnp.dot(xs[...], gbuf[slot], preferred_element_type=F32)
        u = jnp.dot(xs[...], ubuf[slot], preferred_element_type=F32)
        hand_over(j, g, u)
        return g, u

    def cross(d):
        return pltpu.make_async_remote_copy(
            src_ref=whole.at[d], dst_ref=wrecv.at[d], send_sem=cr_ss.at[d],
            recv_sem=cr_rs.at[d], device_id=partner, device_id_type=MESH)

    def project(j, carry):
        @pl.when(j == 1)
        def _():
            pl.semaphore_wait(stage.at[0], ny - 1)

        @pl.when((j > 1) & (j <= nz))
        def _():
            pl.semaphore_wait(stage.at[j - 1], line_count)

        @pl.when(j < nz)
        def _():
            signal_line(stage.at[j])

        multiply(j)
        exchange(j).start()
        fetch_next(j)

        @pl.when(j >= LAG)
        def _():
            finish(j - LAG)
        return carry

    def project_last(j, carry):
        g, u = multiply(j)
        d = j - (STEPS - DIRECT)
        whole[d] = jnp.concatenate([g, u], axis=0).astype(BF16)
        cross(d).start()
        fetch_next(j)
        finish(j - LAG)
        return carry

    lax.fori_loop(1, STEPS - DIRECT, project, 0)
    lax.fori_loop(STEPS - DIRECT, STEPS, project_last, 0)

    nsub = 4
    sw = width // nsub

    def fetch_blocks(k):
        for c in range(per):
            down_b(k * per + c).start()

    def first_part(j, carry):
        @pl.when(j < nz)
        def _():
            fetch_blocks(j)

        share(j).wait_recv()
        down_a(j).wait()
        for q in range(nsub):
            cols = slice(q * sw, (q + 1) * sw)
            y = acc[:, cols]
            for h in range(ny):
                y = y + jnp.dot(hid[j, h], dbuf_a[j, h * hw:(h + 1) * hw, cols],
                                preferred_element_type=F32)
            acc[:, cols] = y

        @pl.when(j < LAG - DIRECT)
        def _():
            finish(STEPS - LAG + j)
        return carry

    lax.fori_loop(0, EARLY, first_part, 0)
    for k in range(EARLY, nz):
        fetch_blocks(k)
    for j in range(EARLY, STEPS):
        d = j - (STEPS - DIRECT)
        if d < 0:
            share(j).wait_recv()
        else:
            cross(d).wait_recv()
        for h in range(ny):
            start = (j - EARLY) * cn + h * hw
            if d < 0:
                late[:, start:start + hw] = hid[j, h]
            else:
                theirs = wrecv[d, :, h * hw:(h + 1) * hw].astype(F32)
                g = part[j, h, 0] + theirs[:ROWS]
                u = part[j, h, 1] + theirs[ROWS:]
                late[:, start:start + hw] = (g * jax.nn.sigmoid(g) * u).astype(BF16)

    def out_copy(i, o):
        _, c, z = block_of(i)
        here = gx * nz + gz
        return pltpu.make_async_remote_copy(
            src_ref=sbuf.at[i, o], dst_ref=rbuf.at[here], send_sem=out_ss.at[i, o],
            recv_sem=out_rs.at[here], device_id=(gy * per + c, o, z), device_id_type=MESH)

    def to_self(i, o):
        _, c, z = block_of(i)
        return (gy * per + c == gx) & (o == gy) & (z == gz)

    def second_part(k, carry):
        for c in range(per):
            down_b(k * per + c).wait()
        y = jnp.dot(late[...], dbuf_b[k], preferred_element_type=F32)
        for c in range(per):
            i = k * per + c
            b, _, _ = block_of(i)
            yc = acc[:, pl.ds(pl.multiple_of(b * bw, 128), bw)] + y[:, c * bw:(c + 1) * bw]
            for o in range(ny):
                sent = jnp.concatenate([yc[o * LOW:(o + 1) * LOW], yc[ny * LOW:]], axis=0).astype(BF16)
                sbuf[i, o] = sent

                @pl.when(to_self(i, o))
                def _():
                    rbuf[gx * nz + gz] = sent

                @pl.when(jnp.logical_not(to_self(i, o)))
                def _():
                    out_copy(i, o).start()
        return carry

    lax.fori_loop(0, nz, second_part, 0)

    src_y = (gx * nz + gz) // nb
    sums = []
    for e in range(nx):
        for z in range(nz):
            @pl.when(jnp.logical_not((e == gx) & (src_y == gy) & (z == gz)))
            def _():
                pltpu.make_async_remote_copy(
                    src_ref=sbuf.at[0, 0], dst_ref=rbuf.at[e * nz + z], send_sem=out_ss.at[0, 0],
                    recv_sem=out_rs.at[e * nz + z], device_id=(e, src_y, z),
                    device_id_type=MESH).wait_recv()
        s = rbuf[e * nz].astype(F32)
        for z in range(1, nz):
            s = s + rbuf[e * nz + z].astype(F32)
        sums.append(jnp.dot(spreads[e], s, precision=lax.Precision.HIGHEST,
                            preferred_element_type=F32))
    out_ref[...] = functools.reduce(lambda a, b: a + b, sums).astype(out_ref.dtype)

    def drain(j, carry):
        exchange(j).wait_send()
        share(j).wait_send()
        return carry

    lax.fori_loop(0, STEPS - DIRECT, drain, 0)
    for d in range(DIRECT):
        cross(d).wait_send()

    def drain_out(i, carry):
        for o in range(ny):
            @pl.when(jnp.logical_not(to_self(i, o)))
            def _():
                out_copy(i, o).wait_send()
        return carry

    lax.fori_loop(0, nb, drain_out, 0)


def fused(sizes, tokens, route, weight_q, w_gate, w_up, w_down):
    nx, ny, nz = sizes
    depth, ffl = w_gate.shape[1], w_gate.shape[2]
    width = w_down.shape[2]
    cn = ffl // STEPS
    hw = cn // ny
    nb = nx * nz // ny
    bw = width // nb
    rest = ffl - EARLY * cn
    dma = pltpu.SemaphoreType.DMA
    hbm = pl.BlockSpec(memory_space=pl.ANY)
    return pl.pallas_call(
        functools.partial(kernel, sizes),
        out_shape=jax.ShapeDtypeStruct((tokens.shape[0], bw), BF16),
        in_specs=[hbm] * 6,
        out_specs=pl.BlockSpec(memory_space=pltpu.VMEM),
        scratch_shapes=[
            pltpu.VMEM(tokens.shape, BF16),
            pltpu.VMEM(route.shape[::-1], jnp.int32),
            pltpu.VMEM(route.shape[::-1], jnp.int32),
            pltpu.VMEM((RING, depth, cn), BF16),
            pltpu.VMEM((RING, depth, cn), BF16),
            pltpu.VMEM((EARLY, cn, width), BF16),
            pltpu.VMEM((nz, rest, nb // nz * bw), BF16),
            pltpu.VMEM((ny, 3, PIECE, depth // 3), BF16),
            pltpu.VMEM((3, PIECE, depth // 3), BF16),
            pltpu.VMEM((ROWS, depth), BF16),
            pltpu.VMEM((STEPS, ny, 2, ROWS, hw), F32),
            pltpu.VMEM((STEPS - DIRECT, 2, ROWS, hw), F32),
            pltpu.VMEM((DIRECT, 2 * ROWS, cn), BF16),
            pltpu.VMEM((DIRECT, 2 * ROWS, cn), BF16),
            pltpu.VMEM((STEPS - DIRECT, ny, ROWS, hw), BF16),
            pltpu.VMEM((ROWS, rest), BF16),
            pltpu.VMEM((ROWS, width), F32),
            pltpu.VMEM((nb, ny, PIECE, bw), BF16),
            pltpu.VMEM((nx * nz, PIECE, bw), BF16),
            dma((3,)), dma((RING,)), dma((RING,)), dma((EARLY,)), dma((nb,)),
            pltpu.SemaphoreType.REGULAR((nz,)),
            dma((3,)), dma((3,)), dma((DIRECT,)), dma((DIRECT,)),
            *[dma((STEPS - DIRECT,))] * 4,
            dma((nb, ny)), dma((nx * nz,)),
        ],
        compiler_params=pltpu.CompilerParams(
            collective_id=0, has_side_effects=True, vmem_limit_bytes=67043328),
        name="routed_ffn",
    )(tokens, route.T, weight_q.T, w_gate, w_up, w_down)


def solution(mesh):
    in_specs = (
        P("gy", None),
        P("gy", None),
        P("gy", None),
        P("gx", "gy", "gz"),
        P("gx", "gy", "gz"),
        P("gx", "gz", "gy"),
    )
    out_specs = P("gy", ("gx", "gz"))
    sizes = tuple(mesh.shape[name] for name in ("gx", "gy", "gz"))
    body = functools.partial(fused, sizes) if sizes[1] == 2 else plain
    return jax.shard_map(
        body, mesh=mesh, in_specs=in_specs, out_specs=out_specs, check_vma=False
    )
```
